32 devices in a mesh: groups: 2 (over x), gx: 16 (over z, y, core).
Axes of the slice: x: 2, y: 2, z: 4, core: 2. Of those that a mesh axis runs over, the one named last changes fastest.
Arguments:
- fields: float32 [3, 1024, 4096], P(None, 'groups', 'gx'), parts along dimension 1, may hold values from -0.7 to 1.4, as said below
- friction: float32 [1024, 4096], P('groups', 'gx'), parts along dimension 0, may hold values from 0.2 to 1.6
- wet_mask: int32 [1024, 4096], P('groups', 'gx'), parts along dimension 0, may hold values from 0 to 1, as said below
- owner_table: int32 [4, 16], P('groups'), parts along dimension 0, may hold values from 0 to 15, as said below
Outputs:
- final_fields: float32 [3, 1024, 4096], P(None, 'groups', 'gx'), parts along dimension 1
- owned_depth: float32 [1024, 4096], P('groups', 'gx'), parts along dimension 0
The draws below stay inside these ranges and needn't reach their ends.
There are 2 independent parts, one for each index of `groups`. The reference program is written for one: setup_inputs(seed, part) draws one part's arguments, and reference() takes and returns one part's arrays. A program takes and returns all parts, laid end to end along the dimension named above; each array names one. Nothing has to cross between parts.
Inputs may be any that keep to these rules, and one draw needn't show every extreme that they name: fields[0] is the depth, 0.6 to 1.4; fields[1] and fields[2] are the momenta, -0.7 to 0.7. `wet_mask`: land covers whole tiles: in each home column the tiles that hold water are the first ones (tile rows 0 up to some row, at least row 0), and some tiles hold no water. In each tile row and each aligned block of 8 home columns, owner_table[r, c] = c XOR k for one k from 0 to 7, so every device owns exactly one tile of each tile row.
All inputs are finite; a program needn't handle non-finite values.
Results may differ from the reference program's by a relative error of at most 0.0003.
Values sent between devices are 32-bit elements; how exact they have to be, the bound alone decides.
No kernel may reach another device: no remote copies, remote signals or barrier semaphores. Data moves between devices by JAX's collectives and lax.ppermute only.
A program may use at most 64 MiB of HBM per device.

```python
import math
import jax
import jax.numpy as jnp
from jax import lax

TILE = 256
TILE_ROWS = 2
STEPS = 2
BLOCK = 8
NR = 512
NC = 4096
N_GX = 16


def coast_layout(key):
    layout_key = jax.random.fold_in(key, 101)
    first_key, second_key, order_key = jax.random.split(layout_key, 3)
    coast_depth = jnp.maximum(jax.random.randint(first_key, (N_GX,), 1, TILE_ROWS + 1) * jax.random.randint(second_key, (N_GX,), 0, 2), 1)
    row_numbers = jnp.arange(TILE_ROWS, dtype=jnp.int32)
    tile_wet = (row_numbers[:, None] < coast_depth[None, :]).astype(jnp.int32)
    block_count = N_GX // BLOCK
    combos = BLOCK ** TILE_ROWS
    combo_index = jnp.arange(combos, dtype=jnp.int32)
    powers = jnp.array([BLOCK ** power_index for power_index in range(TILE_ROWS)], jnp.int32)
    digits = combo_index[:, None] // powers[None, :] % BLOCK
    slot_numbers = jnp.arange(BLOCK, dtype=jnp.int32)
    source = jnp.bitwise_xor(slot_numbers[None, None, :], digits[:, :, None])
    wet_blocks = tile_wet.reshape(TILE_ROWS, block_count, BLOCK).transpose(1, 0, 2)
    spread_wet = jnp.broadcast_to(wet_blocks[:, None], (block_count, combos, TILE_ROWS, BLOCK))
    spread_source = jnp.broadcast_to(source[None], (block_count, combos, TILE_ROWS, BLOCK))
    gathered = jnp.take_along_axis(spread_wet, spread_source, axis=3)
    loads = jnp.max(jnp.sum(gathered, axis=2), axis=2)

    def shuffle(sub_key):
        return jax.random.permutation(sub_key, combos)
    ranks = jax.vmap(shuffle)(jax.random.split(order_key, block_count)).astype(jnp.int32)
    score = loads * combos + ranks
    best = jnp.argmin(score, axis=1)
    chosen_digits = digits[best]
    column_numbers = jnp.arange(N_GX, dtype=jnp.int32)
    owner_rows = jnp.bitwise_xor(column_numbers[None, :], chosen_digits[column_numbers // BLOCK].T)
    return (tile_wet, owner_rows.astype(jnp.int32))


def draw_wet_mask(key, part):
    tile_wet, owner_rows = coast_layout(key)
    cells = jax.random.randint(jax.random.fold_in(key, 202), (TILE_ROWS * TILE, N_GX * TILE), 0, 8)
    spread = jnp.repeat(jnp.repeat(tile_wet, TILE, axis=0), TILE, axis=1)
    return (spread * (cells > 0)).astype(jnp.int32)


def draw_owner_table(key, part):
    tile_wet, owner_rows = coast_layout(key)
    return owner_rows


def draw_fields(key, part):
    row_total = TILE_ROWS * TILE
    column_total = N_GX * TILE
    depth_key, flow_key = jax.random.split(jax.random.fold_in(key, 303))
    rough_depth = jax.random.uniform(depth_key, (row_total, column_total), jnp.float32, -1.0, 1.0)
    rough_flow = jax.random.uniform(flow_key, (2, row_total, column_total), jnp.float32, -1.0, 1.0)
    water = 1.0 + 0.4 * rough_depth
    flows = 0.7 * rough_flow
    return jnp.concatenate([water[None], flows], 0).astype(jnp.float32)


def steps_of(key, shape, cuts, smallest, top_value):
    def one(position, blocks):
        draws = jax.random.uniform(jax.random.fold_in(jax.random.fold_in(key, 6), position), (blocks,), jnp.float32, smallest / len(cuts), top_value / len(cuts))
        return jnp.repeat(jnp.exp(draws), shape[position] // blocks).reshape((-1,) + (1,) * (len(shape) - position - 1))

    level = one(*cuts[0])
    for cut in cuts[1:]:
        level = level * one(*cut)
    return level


def setup_inputs(seed: int = 0, part: int = 0) -> dict:
    streams_of = jax.random.split(jax.random.key(seed), 5)
    part_splits = jax.random.split(jax.random.fold_in(streams_of[4], part), 5)
    return {
        "fields": draw_fields(jax.random.fold_in(jax.random.fold_in(streams_of[4], part), 71), part),
        "friction": jnp.clip(jnp.exp(math.log(1.6) - 2.0794415 * jax.random.uniform(part_splits[1], (NR, NC), jnp.float32) ** steps_of(part_splits[1], (NR, NC), ((1, 16),), -0.2, 0.2)), 0.2, 1.6),
        "wet_mask": draw_wet_mask(jax.random.fold_in(jax.random.fold_in(streams_of[4], part), 71), part),
        "owner_table": draw_owner_table(jax.random.fold_in(jax.random.fold_in(streams_of[4], part), 71), part),
    }


gravity_half = 0.5
depth_floor = 0.25
flux_factor = 0.1
time_step = 0.25


def advance(padded, openness):
    water_depth = padded[0]
    east_flow = padded[1]
    south_flow = padded[2]
    safe_depth = jnp.maximum(water_depth, depth_floor)
    speed_east = east_flow / safe_depth
    speed_south = south_flow / safe_depth
    pressure = gravity_half * water_depth * water_depth
    flux_east = jnp.stack([east_flow, east_flow * speed_east + pressure, south_flow * speed_east])
    flux_south = jnp.stack([south_flow, east_flow * speed_south, south_flow * speed_south + pressure])
    average = 0.25 * (padded[:, 1:-1, 2:] + padded[:, 1:-1, :-2] + padded[:, 2:, 1:-1] + padded[:, :-2, 1:-1])
    update = average - flux_factor * (flux_east[:, 1:-1, 2:] - flux_east[:, 1:-1, :-2]) - flux_factor * (flux_south[:, 2:, 1:-1] - flux_south[:, :-2, 1:-1])
    wet_cells = (openness > 0.0).astype(jnp.float32)
    damping = wet_cells / (1.0 + time_step * openness)
    return jnp.stack([wet_cells * update[0], damping * update[1], damping * update[2]])


def reference(fields, friction, wet_mask, owner_table):
    openness = wet_mask.astype(jnp.float32) * friction
    wet_cells = (openness > 0.0).astype(jnp.float32)
    current = fields * wet_cells[None]
    for step_index in range(STEPS):
        padded = jnp.pad(current, ((0, 0), (1, 1), (1, 1)))

        def column_step(column_index):
            first_cell = (column_index * TILE).astype(jnp.int32)
            block_fields = lax.dynamic_slice_in_dim(padded, first_cell, TILE + 2, 2)
            local_open = lax.dynamic_slice_in_dim(openness, first_cell, TILE, 1)
            return advance(block_fields, local_open)

        pieces = lax.map(column_step, jnp.arange(N_GX, dtype=jnp.int32))
        current = jnp.transpose(pieces, (1, 2, 0, 3)).reshape(3, NR, NC)
    depth_tiles = current[0].reshape(TILE_ROWS, TILE, N_GX, TILE)
    columns = jnp.arange(N_GX, dtype=jnp.int32)
    row_numbers = jnp.arange(TILE_ROWS, dtype=jnp.int32)
    inverse = jnp.zeros((TILE_ROWS, N_GX), jnp.int32).at[row_numbers[:, None], owner_table].set(jnp.broadcast_to(columns[None, :], (TILE_ROWS, N_GX)))
    index_table = jnp.broadcast_to(inverse[:, None, :, None], (TILE_ROWS, TILE, N_GX, TILE))
    owned_depth = jnp.take_along_axis(depth_tiles, index_table, axis=2).reshape(NR, NC)
    return current, owned_depth
```

```python
from functools import partial

import jax
import jax.numpy as jnp
from jax import lax
from jax.experimental import pallas as pl
from jax.experimental.pallas import tpu as pltpu
from jax.sharding import PartitionSpec as P

STEPS = 2
LEVELS = 3
LANES = 128
SUBLANES = 8
GROUPS_PER_TRIP = 4
SLOT = 16
VMEM_BYTES = 16 * 1024 * 1024

depth_floor = 0.25
flux_factor = 0.1
time_step = 0.25

VMEM = pl.BlockSpec(memory_space=pltpu.VMEM)
PARAMS = pltpu.CompilerParams(vmem_limit_bytes=VMEM_BYTES)


def flux_terms(depth, east, south):
    inverse = 1.0 / jnp.maximum(depth, depth_floor)
    speed_east = (flux_factor * inverse) * east
    speed_south = (flux_factor * inverse) * south
    pressure = (0.5 * flux_factor) * depth * depth
    cross = south * speed_east
    flux_east = (flux_factor * east, east * speed_east + pressure, cross)
    flux_south = (flux_factor * south, cross, south * speed_south + pressure)
    quarter = (0.25 * depth, 0.25 * east, 0.25 * south)
    from_east = [a - f for a, f in zip(quarter, flux_east)]
    from_west = [a + f for a, f in zip(quarter, flux_east)]
    from_south = [a - g for a, g in zip(quarter, flux_south)]
    from_north = [a + g for a, g in zip(quarter, flux_south)]
    return from_east, from_west, from_south, from_north


def pack_kernel(fields, friction, wet_mask, edges, pay_pair, pay_other, rows):
    width = fields.shape[2]
    height = fields.shape[1]
    lane = lax.broadcasted_iota(jnp.int32, (height, LANES), 1)
    packed = jnp.zeros((height, LANES), jnp.float32)
    openness = []
    for first in (0, width - LANES):
        span = slice(first, first + LANES)
        openness.append(wet_mask[:, span].astype(jnp.float32) * friction[:, span])
    for index in range(4):
        for side in range(2):
            span = slice(0, LANES) if side == 0 else slice(width - LANES, width)
            if index < 3:
                value = fields[index, :, span] * (openness[side] > 0.0).astype(jnp.float32)
            else:
                value = openness[side]
            start = index * SLOT + (2 if side == 0 else SUBLANES + 2)
            source = 0 if side == 0 else LANES - 4
            turned = pltpu.roll(value, (start - source) % LANES, 1)
            packed = jnp.where((lane >= start) & (lane < start + 4), turned, packed)
    for block in range(height // LANES):
        span = slice(block * LANES, (block + 1) * LANES)
        rows[:, span] = packed[span].T
    edges[...] = rows[0 : 4 * SLOT]
    even = lax.rem(lax.axis_index("gx"), 2) == 0
    for index in range(4):
        for far in range(2):
            left = rows[pl.ds(index * SLOT + 2 + far, 1), :]
            right = rows[pl.ds(index * SLOT + SUBLANES + 5 - far, 1), :]
            pay_pair[pl.ds(4 * far + index, 1), :] = jnp.where(even, right, left)
            pay_other[pl.ds(4 * far + index, 1), :] = jnp.where(even, left, right)


def main_kernel(fields, friction, wet_mask, result, middle, damp):
    height, width = fields.shape[1], fields.shape[2]
    groups = height // SUBLANES
    sub = lax.broadcasted_iota(jnp.int32, (SUBLANES, width), 0)
    zero = jnp.zeros((SUBLANES, width), jnp.float32)

    def sweep(load, store):
        def finish(held, south_now):
            return [h + jnp.where(sub == SUBLANES - 1, s, 0.0) for h, s in zip(held, south_now)]

        def trip(i, carry):
            held, north_last = carry
            for j in range(GROUPS_PER_TRIP):
                group = i * GROUPS_PER_TRIP + j
                from_east, from_west, from_south, from_north = flux_terms(*load(group))
                across = [
                    pltpu.roll(e, width - 1, 1) + pltpu.roll(w, 1, 1)
                    for e, w in zip(from_east, from_west)
                ]
                south_now = [pltpu.roll(s, SUBLANES - 1, 0) for s in from_south]
                north_now = [pltpu.roll(n, 1, 0) for n in from_north]
                store(jnp.maximum(group - 1, 0), finish(held, south_now))
                held = [
                    a + jnp.where(sub == SUBLANES - 1, 0.0, s) + jnp.where(sub == 0, last, n)
                    for a, s, last, n in zip(across, south_now, north_last, north_now)
                ]
                north_last = north_now
            return held, north_last

        held, _ = lax.fori_loop(
            0, groups // GROUPS_PER_TRIP, trip, ([zero] * 3, [zero] * 3)
        )
        store(groups - 1, held)

    def rows_of(group):
        start = group * SUBLANES
        if not isinstance(start, int):
            start = pl.multiple_of(start, SUBLANES)
        return pl.ds(start, SUBLANES)

    def load_first(group):
        rows = rows_of(group)
        openness = wet_mask[rows, :].astype(jnp.float32) * friction[rows, :]
        wet = (openness > 0.0).astype(jnp.float32)
        damp[0, rows, :] = wet
        damp[1, rows, :] = wet / (1.0 + time_step * openness)
        return [fields[c, rows, :] * wet for c in range(3)]

    def load_second(group):
        return [middle[c, rows_of(group), :] for c in range(3)]

    def store_into(target):
        def store(group, update):
            rows = rows_of(group)
            for c in range(3):
                target[c, rows, :] = damp[min(c, 1), rows, :] * update[c]

        return store

    sweep(load_first, store_into(middle))
    sweep(load_second, store_into(result))


def edge_kernel(edges, got_pair, got_other, unfinished, result, rows):
    height, width = unfinished.shape[1], unfinished.shape[2]
    rows[0 : 4 * SLOT] = edges[...]
    even = lax.rem(lax.axis_index("gx"), 2) == 0
    for index in range(4):
        for far in range(2):
            pair = got_pair[pl.ds(4 * far + index, 1), :]
            other = got_other[pl.ds(4 * far + index, 1), :]
            rows[pl.ds(index * SLOT + 1 - far, 1), :] = jnp.where(even, other, pair)
            rows[pl.ds(index * SLOT + SUBLANES + 6 + far, 1), :] = jnp.where(even, pair, other)
    lane = lax.broadcasted_iota(jnp.int32, (SLOT, height), 1)
    state = [rows[c * SLOT : (c + 1) * SLOT] for c in range(3)]
    openness = rows[3 * SLOT : 4 * SLOT]
    wet = (openness > 0.0).astype(jnp.float32)
    damping = wet / (1.0 + time_step * openness)
    for _ in range(STEPS):
        from_east, from_west, from_south, from_north = flux_terms(*state)
        update = [
            pltpu.roll(e, SLOT - 1, 0)
            + pltpu.roll(w, 1, 0)
            + jnp.where(lane == height - 1, 0.0, pltpu.roll(s, height - 1, 1))
            + jnp.where(lane == 0, 0.0, pltpu.roll(n, 1, 1))
            for e, w, s, n in zip(from_east, from_west, from_south, from_north)
        ]
        state = [wet * update[0], damping * update[1], damping * update[2]]
    lane = lax.broadcasted_iota(jnp.int32, (LANES, LANES), 1)
    rows[...] = jnp.zeros_like(rows)
    for c in range(3):
        rows[c * SLOT : (c + 1) * SLOT] = state[c]
    for block in range(height // LANES):
        span = slice(block * LANES, (block + 1) * LANES)
        columns = rows[:, span].T
        for c in range(3):
            left = pltpu.roll(columns, (-(c * SLOT + 2)) % LANES, 1)
            right = pltpu.roll(columns, (LANES - 2 - (c * SLOT + SUBLANES + 4)) % LANES, 1)
            result[c, span, 0:LANES] = jnp.where(lane < 2, left, unfinished[c, span, 0:LANES])
            result[c, span, width - LANES : width] = jnp.where(
                lane >= LANES - 2, right, unfinished[c, span, width - LANES : width]
            )


def direct(top, bottom, first, second):
    def move(tile, distance):
        if distance == 0:
            return tile
        count = lax.axis_size("gx")
        return lax.ppermute(tile, "gx", [(i, i ^ distance) for i in range(count)])

    return move(top, first), move(bottom, second)


def body(fields, friction, wet_mask, owner_table):
    _, height, width = fields.shape
    count = lax.axis_size("gx")
    column = lax.axis_index("gx")
    tile_rows = height // width
    own = lax.dynamic_slice_in_dim(owner_table, column, 1, 1)[:, 0]
    keys = jnp.bitwise_xor(own, column)
    distances = 1 << LEVELS
    choice = keys[0] * distances + keys[1]

    f32 = jnp.float32
    edges, pay_pair, pay_other = pl.pallas_call(
        pack_kernel,
        out_shape=[
            jax.ShapeDtypeStruct((4 * SLOT, height), f32),
            jax.ShapeDtypeStruct((SUBLANES, height), f32),
            jax.ShapeDtypeStruct((SUBLANES, height), f32),
        ],
        in_specs=[VMEM] * 3,
        out_specs=[VMEM] * 3,
        scratch_shapes=[pltpu.VMEM((LANES, height), f32)],
        compiler_params=PARAMS,
        name="pack",
    )(fields, friction, wet_mask)
    got_pair = lax.ppermute(pay_pair, "gx", [(i, i ^ 1) for i in range(count)])
    others = [(i, i + 1) for i in range(1, count - 1, 2)]
    got_other = lax.ppermute(pay_other, "gx", others + [(b, a) for a, b in others])
    unfinished = pl.pallas_call(
        main_kernel,
        out_shape=jax.ShapeDtypeStruct(fields.shape, f32),
        in_specs=[VMEM] * 3,
        out_specs=VMEM,
        scratch_shapes=[pltpu.VMEM(fields.shape, f32), pltpu.VMEM((2, height, width), f32)],
        compiler_params=PARAMS,
        cost_estimate=pl.CostEstimate(
            flops=200 * 3 * height * width, bytes_accessed=16 * height * width, transcendentals=0
        ),
        name="both_steps",
    )(fields, friction, wet_mask)
    final_fields = pl.pallas_call(
        edge_kernel,
        out_shape=jax.ShapeDtypeStruct(fields.shape, f32),
        in_specs=[VMEM] * 4,
        out_specs=VMEM,
        scratch_shapes=[pltpu.VMEM((LANES, height), f32)],
        compiler_params=PARAMS,
        name="edge_columns",
    )(edges, got_pair, got_other, unfinished)
    depth = final_fields[0].reshape(tile_rows, width, width)
    moved = lax.switch(
        choice,
        [
            partial(direct, first=first, second=second)
            for first in range(distances)
            for second in range(distances)
        ],
        depth[0],
        depth[1],
    )
    owned_depth = jnp.concatenate(moved, axis=0)
    return final_fields, owned_depth


def solution(mesh):
    in_specs = (P(None, "groups", "gx"), P("groups", "gx"), P("groups", "gx"), P("groups", None))
    out_specs = (P(None, "groups", "gx"), P("groups", "gx"))
    return jax.shard_map(body, mesh=mesh, in_specs=in_specs, out_specs=out_specs, check_vma=False)
```

```python
from functools import partial

import jax
import jax.numpy as jnp
from jax import lax
from jax.experimental import pallas as pl
from jax.experimental.pallas import tpu as pltpu
from jax.sharding import PartitionSpec as P

STEPS = 2
LEVELS = 3
LANES = 128
SUBLANES = 8
UNROLL = 16
SLOT = 16
KEEP = 4
VMEM_BYTES = 16 * 1024 * 1024

depth_floor = 0.25
flux_factor = 0.1
time_step = 0.25

VMEM = pl.BlockSpec(memory_space=pltpu.VMEM)
SMEM = pl.BlockSpec(memory_space=pltpu.SMEM)
HBM = pl.BlockSpec(memory_space=pltpu.HBM)
PARAMS = pltpu.CompilerParams(vmem_limit_bytes=VMEM_BYTES)


def flux_terms(depth, east, south):
    inverse = flux_factor / jnp.maximum(depth, depth_floor)
    speed_east = inverse * east
    speed_south = inverse * south
    pressure = (0.5 * flux_factor) * depth * depth
    cross = south * speed_east
    flux_east = (flux_factor * east, east * speed_east + pressure, cross)
    flux_south = (flux_factor * south, cross, south * speed_south + pressure)
    quarter = (0.25 * depth, 0.25 * east, 0.25 * south)
    from_east = [a - f for a, f in zip(quarter, flux_east)]
    from_west = [a + f for a, f in zip(quarter, flux_east)]
    from_south = [a - g for a, g in zip(quarter, flux_south)]
    from_north = [a + g for a, g in zip(quarter, flux_south)]
    return from_east, from_west, from_south, from_north


def pack_kernel(
    fields_in, friction_in, mask_in, table_in,
    fields, friction, wet_mask, turned, pay_pair, pay_other, choice,
    table, arrived, told,
):
    height, width = fields.shape[1], fields.shape[2]
    count = height // LANES
    read_table = pltpu.make_async_copy(table_in, table, told)
    read_table.start()
    copies = []
    for block in range(count):
        span = pl.ds(block * LANES, LANES)
        copies.append(
            [
                pltpu.make_async_copy(fields_in.at[:, span], fields.at[:, span], arrived.at[block, 0]),
                pltpu.make_async_copy(friction_in.at[span], friction.at[span], arrived.at[block, 1]),
                pltpu.make_async_copy(mask_in.at[span], wet_mask.at[span], arrived.at[block, 2]),
            ]
        )
        for copy in copies[-1]:
            copy.start()
    lane = lax.broadcasted_iota(jnp.int32, (LANES, LANES), 1)
    ends = (slice(0, LANES), slice(width - LANES, width))

    def outer(left, right):
        return jnp.where(lane < KEEP, left, right)

    for block in range(count):
        for copy in copies[block]:
            copy.wait()
        span = slice(block * LANES, (block + 1) * LANES)
        openness = outer(
            *[wet_mask[span, end].astype(jnp.float32) * friction[span, end] for end in ends]
        )
        wet = (openness > 0.0).astype(jnp.float32)
        packed = openness
        for c in range(3):
            value = outer(*[fields[c, span, end] for end in ends]) * wet
            value = pltpu.roll(value, (c - 3) * SUBLANES % LANES, 1)
            start = (c - 3) * SUBLANES - KEEP + LANES
            packed = jnp.where((lane >= start) & (lane < start + SUBLANES), value, packed)
        packed = pltpu.roll(packed, 3 * SUBLANES + KEEP, 1)
        turned[:, span] = packed.T[0 : 4 * SUBLANES]
    even = lax.rem(lax.axis_index("gx"), 2) == 0
    for index in range(4):
        for far in range(2):
            right = turned[pl.ds(index * SUBLANES + KEEP - 1 - far, 1), :]
            left = turned[pl.ds(index * SUBLANES + KEEP + far, 1), :]
            pay_pair[pl.ds(4 * far + index, 1), :] = jnp.where(even, right, left)
            pay_other[pl.ds(4 * far + index, 1), :] = jnp.where(even, left, right)
    read_table.wait()
    column = lax.axis_index("gx")
    key = 0
    for tile_row in range(table.shape[0]):
        key = (key << LEVELS) + (table[tile_row, column] ^ column)
    choice[0] = key


def main_kernel(fields, friction, wet_mask, result, middle, damp, south, north):
    height, width = fields.shape[1], fields.shape[2]
    groups = height // SUBLANES
    tiles = width // LANES
    lane = lax.broadcasted_iota(jnp.int32, (SUBLANES, LANES), 1)
    first_lane, last_lane = lane == 0, lane == LANES - 1
    zero = jnp.zeros((SUBLANES, LANES), jnp.float32)
    for c in range(3):
        for t in range(tiles):
            north[c, t, 0:SUBLANES] = zero
            south[c, t, height : height + SUBLANES] = zero

    def rows_of(group, offset=0):
        start = group * SUBLANES
        if not isinstance(start, int):
            start = pl.multiple_of(start, SUBLANES)
        return pl.ds(start + offset, SUBLANES)

    def across(from_east, from_west):
        east = [pltpu.roll(x, LANES - 1, 1) for x in from_east]
        west = [pltpu.roll(x, 1, 1) for x in from_west]
        return [
            jnp.where(last_lane, east[(t + 1) % tiles], east[t])
            + jnp.where(first_lane, west[t - 1], west[t])
            for t in range(tiles)
        ]

    def sweep(load, store):
        def finish(group, held):
            for t in range(tiles):
                store(
                    group, t, [held[c][t] + south[c, t, rows_of(group, 1)] for c in range(3)]
                )

        def one(group, held):
            per_tile = [flux_terms(*state) for state in load(group)]
            for t in range(tiles):
                for c in range(3):
                    south[c, t, rows_of(group)] = per_tile[t][2][c]
                    north[c, t, rows_of(group + 1)] = per_tile[t][3][c]
            finish(jnp.maximum(group - 1, 0), held)
            held = []
            for c in range(3):
                side = across([x[0][c] for x in per_tile], [x[1][c] for x in per_tile])
                held.append(
                    [side[t] + north[c, t, rows_of(group, SUBLANES - 1)] for t in range(tiles)]
                )
            return held

        def trip(i, held):
            for j in range(UNROLL):
                held = one(i * UNROLL + j, held)
            return held

        held = lax.fori_loop(0, groups // UNROLL, trip, [[zero] * tiles] * 3)
        finish(groups - 1, held)

    def load_first(group):
        states = []
        for t in range(tiles):
            span = (rows_of(group), slice(t * LANES, (t + 1) * LANES))
            openness = wet_mask[span].astype(jnp.float32) * friction[span]
            wet = (openness > 0.0).astype(jnp.float32)
            damp[(0, *span)] = wet
            damp[(1, *span)] = wet / (1.0 + time_step * openness)
            states.append([fields[(c, *span)] * wet for c in range(3)])
        return states

    def load_second(group):
        return [
            [middle[c, rows_of(group), t * LANES : (t + 1) * LANES] for c in range(3)]
            for t in range(tiles)
        ]

    def store_into(target):
        def store(group, t, update):
            span = (rows_of(group), slice(t * LANES, (t + 1) * LANES))
            for c in range(3):
                target[(c, *span)] = damp[(min(c, 1), *span)] * update[c]

        return store

    sweep(load_first, store_into(middle))
    sweep(load_second, store_into(result))


def edge_kernel(turned, got_pair, got_other, unfinished, top, bottom, columns, rows):
    height, width = unfinished.shape[1], unfinished.shape[2]
    rows[...] = jnp.zeros_like(rows)
    even = lax.rem(lax.axis_index("gx"), 2) == 0
    for index in range(4):
        start = index * SLOT
        own = index * SUBLANES
        rows[start : start + KEEP] = turned[own : own + KEEP]
        rows[start + SLOT - KEEP : start + SLOT] = turned[own + KEEP : own + 2 * KEEP]
        for far in range(2):
            pair = got_pair[pl.ds(4 * far + index, 1), :]
            other = got_other[pl.ds(4 * far + index, 1), :]
            rows[pl.ds(start + SLOT - KEEP - 1 - far, 1), :] = jnp.where(even, other, pair)
            rows[pl.ds(start + KEEP + far, 1), :] = jnp.where(even, pair, other)
    lane = lax.broadcasted_iota(jnp.int32, (SLOT, height), 1)
    state = [rows[c * SLOT : (c + 1) * SLOT] for c in range(3)]
    openness = rows[3 * SLOT : 4 * SLOT]
    wet = (openness > 0.0).astype(jnp.float32)
    damping = wet / (1.0 + time_step * openness)
    for _ in range(STEPS):
        from_east, from_west, from_south, from_north = flux_terms(*state)
        update = [
            pltpu.roll(e, SLOT - 1, 0)
            + pltpu.roll(w, 1, 0)
            + jnp.where(lane == height - 1, 0.0, pltpu.roll(s, height - 1, 1))
            + jnp.where(lane == 0, 0.0, pltpu.roll(n, 1, 1))
            for e, w, s, n in zip(from_east, from_west, from_south, from_north)
        ]
        state = [wet * update[0], damping * update[1], damping * update[2]]
    for c in range(3):
        last = (4 * c - 2) % LANES
        rows[last : last + 2] = state[c][KEEP - 2 : KEEP]
        rows[4 * c : 4 * c + 2] = state[c][SLOT - KEEP : SLOT - KEEP + 2]
    lane = lax.broadcasted_iota(jnp.int32, (LANES, LANES), 1)
    for block in range(height // LANES):
        span = slice(block * LANES, (block + 1) * LANES)
        turned_back = rows[:, span].T
        columns[span] = turned_back
        target, first = (top, 0) if block * LANES < width else (bottom, width)
        for end, chosen in ((0, lane < 2), (width - LANES, lane >= LANES - 2)):
            target[block * LANES - first : (block + 1) * LANES - first, end : end + LANES] = (
                jnp.where(chosen, turned_back, unfinished[0, span, end : end + LANES])
            )


def finish_kernel(top, bottom, columns, unfinished, result, momenta, sent):
    height, width = unfinished.shape[1], unfinished.shape[2]
    copies = [
        pltpu.make_async_copy(top, result.at[0, 0:width], sent.at[0]),
        pltpu.make_async_copy(bottom, result.at[0, width:height], sent.at[1]),
    ]
    for copy in copies:
        copy.start()
    lane = lax.broadcasted_iota(jnp.int32, (SUBLANES, LANES), 1)
    for c in range(2):

        def trip(i, carry):
            span = pl.ds(pl.multiple_of(i * SUBLANES, SUBLANES), SUBLANES)
            value = pltpu.roll(columns[span, :], LANES - 4 * (c + 1), 1)
            for end, chosen in ((0, lane < 2), (width - LANES, lane >= LANES - 2)):
                momenta[c, span, end : end + LANES] = jnp.where(
                    chosen, value, unfinished[c + 1, span, end : end + LANES]
                )
            return carry

        lax.fori_loop(0, height // SUBLANES, trip, 0, unroll=8)
        copies.append(pltpu.make_async_copy(momenta.at[c], result.at[c + 1], sent.at[c + 2]))
        copies[-1].start()
    for copy in copies:
        copy.wait()


def place_kernel(top, bottom, result, sent):
    side = top.shape[0]
    copies = [
        pltpu.make_async_copy(top, result.at[0:side], sent.at[0]),
        pltpu.make_async_copy(bottom, result.at[side : 2 * side], sent.at[1]),
    ]
    for copy in copies:
        copy.start()
    for copy in copies:
        copy.wait()


def direct(top, bottom, columns, unfinished, first, second):
    def move(tile, distance):
        if distance == 0:
            return tile
        count = lax.axis_size("gx")
        return lax.ppermute(tile, "gx", [(i, i ^ distance) for i in range(count)])

    moved = move(top, first), move(bottom, second)
    final_fields = pl.pallas_call(
        finish_kernel,
        out_shape=pltpu.HBM(unfinished.shape, jnp.float32),
        in_specs=[VMEM] * 4,
        out_specs=HBM,
        scratch_shapes=[
            pltpu.VMEM((2, *unfinished.shape[1:]), jnp.float32),
            pltpu.SemaphoreType.DMA((4,)),
        ],
        compiler_params=PARAMS,
        cost_estimate=pl.CostEstimate(
            flops=10**7, bytes_accessed=8 * unfinished.size, transcendentals=0
        ),
        name="finish",
    )(top, bottom, columns, unfinished)
    return (*moved, final_fields)


def in_hbm(x):
    return pltpu.with_memory_space_constraint(x, pltpu.HBM)


def body(fields, friction, wet_mask, owner_table):
    _, height, width = fields.shape
    count = lax.axis_size("gx")
    distances = 1 << LEVELS
    blocks = height // LANES
    f32 = jnp.float32
    row_payload = jax.ShapeDtypeStruct((SUBLANES, height), f32)
    fields, friction, wet_mask, turned, pay_pair, pay_other, choice = pl.pallas_call(
        pack_kernel,
        out_shape=[
            jax.ShapeDtypeStruct(fields.shape, f32),
            jax.ShapeDtypeStruct(friction.shape, f32),
            jax.ShapeDtypeStruct(wet_mask.shape, jnp.int32),
            jax.ShapeDtypeStruct((4 * SUBLANES, height), f32),
            row_payload,
            row_payload,
            jax.ShapeDtypeStruct((1,), jnp.int32),
        ],
        in_specs=[HBM] * 4,
        out_specs=[VMEM] * 6 + [SMEM],
        scratch_shapes=[
            pltpu.SMEM(owner_table.shape, jnp.int32),
            pltpu.SemaphoreType.DMA((blocks, 3)),
            pltpu.SemaphoreType.DMA,
        ],
        compiler_params=PARAMS,
        name="pack",
    )(*[in_hbm(x) for x in (fields, friction, wet_mask, owner_table)])
    got_pair = lax.ppermute(pay_pair, "gx", [(i, i ^ 1) for i in range(count)])
    others = [(i, i + 1) for i in range(1, count - 1, 2)]
    got_other = lax.ppermute(pay_other, "gx", others + [(b, a) for a, b in others])
    unfinished = pl.pallas_call(
        main_kernel,
        out_shape=jax.ShapeDtypeStruct(fields.shape, f32),
        in_specs=[VMEM] * 3,
        out_specs=VMEM,
        scratch_shapes=[
            pltpu.VMEM(fields.shape, f32),
            pltpu.VMEM((2, height, width), f32),
            pltpu.VMEM((3, width // LANES, height + SUBLANES, LANES), f32),
            pltpu.VMEM((3, width // LANES, height + SUBLANES, LANES), f32),
        ],
        compiler_params=PARAMS,
        cost_estimate=pl.CostEstimate(
            flops=200 * fields.size, bytes_accessed=16 * height * width, transcendentals=0
        ),
        name="both_steps",
    )(fields, friction, wet_mask)
    tile = jax.ShapeDtypeStruct((width, width), f32)
    top, bottom, columns = pl.pallas_call(
        edge_kernel,
        out_shape=[tile, tile, jax.ShapeDtypeStruct((height, LANES), f32)],
        in_specs=[VMEM] * 4,
        out_specs=[VMEM] * 3,
        scratch_shapes=[pltpu.VMEM((LANES, height), f32)],
        compiler_params=PARAMS,
        name="edge_columns",
    )(turned, got_pair, got_other, unfinished)
    top, bottom, final_fields = lax.switch(
        choice[0],
        [
            partial(direct, first=first, second=second)
            for first in range(distances)
            for second in range(distances)
        ],
        top,
        bottom,
        columns,
        unfinished,
    )
    owned_depth = pl.pallas_call(
        place_kernel,
        out_shape=pltpu.HBM((height, width), f32),
        in_specs=[VMEM] * 2,
        out_specs=HBM,
        scratch_shapes=[pltpu.SemaphoreType.DMA((2,))],
        compiler_params=PARAMS,
        name="place",
    )(top, bottom)
    return final_fields, owned_depth


def solution(mesh):
    in_specs = (P(None, "groups", "gx"), P("groups", "gx"), P("groups", "gx"), P("groups", None))
    out_specs = (P(None, "groups", "gx"), P("groups", "gx"))
    return jax.shard_map(body, mesh=mesh, in_specs=in_specs, out_specs=out_specs, check_vma=False)
```

```python
from functools import partial

import jax
import jax.numpy as jnp
from jax import lax
from jax.experimental import pallas as pl
from jax.experimental.pallas import tpu as pltpu
from jax.sharding import PartitionSpec as P

STEPS = 2
LEVELS = 3
LANES = 128
SUBLANES = 8
UNROLL = 16
FEW = 4
SLOT = 16
KEEP = 4
VMEM_BYTES = 16 * 1024 * 1024

depth_floor = 0.25
flux_factor = 0.1
time_step = 0.25

VMEM = pl.BlockSpec(memory_space=pltpu.VMEM)
HBM = pl.BlockSpec(memory_space=pltpu.HBM)
PARAMS = pltpu.CompilerParams(vmem_limit_bytes=VMEM_BYTES)


def flux_terms(depth, east, south):
    inverse = flux_factor / jnp.maximum(depth, depth_floor)
    speed_east = inverse * east
    speed_south = inverse * south
    pressure = (0.5 * flux_factor) * depth * depth
    cross = south * speed_east
    flux_east = (flux_factor * east, east * speed_east + pressure, cross)
    flux_south = (flux_factor * south, cross, south * speed_south + pressure)
    quarter = (0.25 * depth, 0.25 * east, 0.25 * south)
    from_east = [a - f for a, f in zip(quarter, flux_east)]
    from_west = [a + f for a, f in zip(quarter, flux_east)]
    from_south = [a - g for a, g in zip(quarter, flux_south)]
    from_north = [a + g for a, g in zip(quarter, flux_south)]
    return from_east, from_west, from_south, from_north


def pack_kernel(
    fields_in, friction_in, mask_in, table_in,
    fields, friction, wet_mask, turned, pay_pair, pay_other, choice,
    table, key_cell, arrived, told,
):
    height, width = fields.shape[1], fields.shape[2]
    count = height // LANES
    read_table = pltpu.make_async_copy(table_in, table, told)
    read_table.start()
    copies = []
    for block in range(count):
        span = pl.ds(block * LANES, LANES)
        copies.append(
            [
                pltpu.make_async_copy(fields_in.at[:, span], fields.at[:, span], arrived.at[block, 0]),
                pltpu.make_async_copy(friction_in.at[span], friction.at[span], arrived.at[block, 1]),
                pltpu.make_async_copy(mask_in.at[span], wet_mask.at[span], arrived.at[block, 2]),
            ]
        )
        for copy in copies[-1]:
            copy.start()
    read_table.wait()
    column = lax.axis_index("gx")
    key = 0
    for tile_row in range(table.shape[0]):
        key = (key << LEVELS) + (table[tile_row, column] ^ column)
    key_cell[0] = key
    write_key = pltpu.make_async_copy(key_cell, choice, told)
    write_key.start()
    lane = lax.broadcasted_iota(jnp.int32, (LANES, LANES), 1)
    ends = (slice(0, LANES), slice(width - LANES, width))

    def outer(left, right):
        return jnp.where(lane < KEEP, left, right)

    for block in range(count):
        for copy in copies[block]:
            copy.wait()
        span = slice(block * LANES, (block + 1) * LANES)
        openness = outer(
            *[wet_mask[span, end].astype(jnp.float32) * friction[span, end] for end in ends]
        )
        wet = (openness > 0.0).astype(jnp.float32)
        packed = openness
        for c in range(3):
            value = outer(*[fields[c, span, end] for end in ends]) * wet
            value = pltpu.roll(value, (c - 3) * SUBLANES % LANES, 1)
            start = (c - 3) * SUBLANES - KEEP + LANES
            packed = jnp.where((lane >= start) & (lane < start + SUBLANES), value, packed)
        packed = pltpu.roll(packed, 3 * SUBLANES + KEEP, 1)
        turned[:, span] = packed.T[0 : 4 * SUBLANES]
    even = lax.rem(lax.axis_index("gx"), 2) == 0
    for index in range(4):
        for far in range(2):
            right = turned[pl.ds(index * SUBLANES + KEEP - 1 - far, 1), :]
            left = turned[pl.ds(index * SUBLANES + KEEP + far, 1), :]
            pay_pair[pl.ds(4 * far + index, 1), :] = jnp.where(even, right, left)
            pay_other[pl.ds(4 * far + index, 1), :] = jnp.where(even, left, right)
    write_key.wait()


def rows_of(group, offset=0):
    start = group * SUBLANES
    if not isinstance(start, int):
        start = pl.multiple_of(start, SUBLANES)
    return pl.ds(start + offset, SUBLANES)


def sweep(height, width, parts, unroll, load, store, south, north):
    groups = height // SUBLANES
    tiles = width // LANES
    lane = lax.broadcasted_iota(jnp.int32, (SUBLANES, LANES), 1)
    first_lane, last_lane = lane == 0, lane == LANES - 1
    zero = jnp.zeros((SUBLANES, LANES), jnp.float32)
    for i in range(len(parts)):
        for t in range(tiles):
            north[i, t, 0:SUBLANES] = zero
            south[i, t, height : height + SUBLANES] = zero

    def across(from_east, from_west):
        east = [pltpu.roll(x, LANES - 1, 1) for x in from_east]
        west = [pltpu.roll(x, 1, 1) for x in from_west]
        return [
            jnp.where(last_lane, east[(t + 1) % tiles], east[t])
            + jnp.where(first_lane, west[t - 1], west[t])
            for t in range(tiles)
        ]

    def finish(group, held):
        for t in range(tiles):
            below = [south[i, t, rows_of(group, 1)] for i in range(len(parts))]
            store(group, t, [held[i][t] + below[i] for i in range(len(parts))])

    def one(group, held):
        per_tile = [flux_terms(*state) for state in load(group)]
        for t in range(tiles):
            for i, part in enumerate(parts):
                south[i, t, rows_of(group)] = per_tile[t][2][part]
                north[i, t, rows_of(group + 1)] = per_tile[t][3][part]
        finish(jnp.maximum(group - 1, 0), held)
        held = []
        for i, part in enumerate(parts):
            side = across([x[0][part] for x in per_tile], [x[1][part] for x in per_tile])
            held.append([side[t] + north[i, t, rows_of(group, SUBLANES - 1)] for t in range(tiles)])
        return held

    def trip(k, held):
        for j in range(unroll):
            held = one(k * unroll + j, held)
        return held

    held = lax.fori_loop(0, groups // unroll, trip, [[zero] * tiles] * len(parts))
    finish(groups - 1, held)


def tile_span(group, t):
    return (rows_of(group), slice(t * LANES, (t + 1) * LANES))


def load_state(middle, group):
    tiles = middle.shape[2] // LANES
    return [[middle[(c, *tile_span(group, t))] for c in range(3)] for t in range(tiles)]


def main_kernel(fields, friction, wet_mask, depth, middle, damping, wet_cells, south, north):
    height, width = depth.shape
    tiles = width // LANES

    def load(group):
        states = []
        for t in range(tiles):
            span = tile_span(group, t)
            openness = wet_mask[span].astype(jnp.float32) * friction[span]
            wet = (openness > 0.0).astype(jnp.float32)
            wet_cells[span] = wet
            damping[span] = wet / (1.0 + time_step * openness)
            states.append([fields[(c, *span)] * wet for c in range(3)])
        return states

    def store(group, t, update):
        span = tile_span(group, t)
        damp = damping[span]
        middle[(0, *span)] = wet_cells[span] * update[0]
        middle[(1, *span)] = damp * update[1]
        middle[(2, *span)] = damp * update[2]

    def store_depth(group, t, update):
        span = tile_span(group, t)
        depth[span] = wet_cells[span] * update[0]

    sweep(height, width, (0, 1, 2), UNROLL, load, store, south, north)
    sweep(height, width, (0,), UNROLL, partial(load_state, middle), store_depth, south, north)


def edge_kernel(turned, got_pair, got_other, depth, top, bottom, columns, rows):
    height, width = depth.shape
    rows[...] = jnp.zeros_like(rows)
    even = lax.rem(lax.axis_index("gx"), 2) == 0
    for index in range(4):
        start = index * SLOT
        own = index * SUBLANES
        rows[start : start + KEEP] = turned[own : own + KEEP]
        rows[start + SLOT - KEEP : start + SLOT] = turned[own + KEEP : own + 2 * KEEP]
        for far in range(2):
            pair = got_pair[pl.ds(4 * far + index, 1), :]
            other = got_other[pl.ds(4 * far + index, 1), :]
            rows[pl.ds(start + SLOT - KEEP - 1 - far, 1), :] = jnp.where(even, other, pair)
            rows[pl.ds(start + KEEP + far, 1), :] = jnp.where(even, pair, other)
    lane = lax.broadcasted_iota(jnp.int32, (SLOT, height), 1)
    state = [rows[c * SLOT : (c + 1) * SLOT] for c in range(3)]
    openness = rows[3 * SLOT : 4 * SLOT]
    wet = (openness > 0.0).astype(jnp.float32)
    damping = wet / (1.0 + time_step * openness)
    for _ in range(STEPS):
        from_east, from_west, from_south, from_north = flux_terms(*state)
        update = [
            pltpu.roll(e, SLOT - 1, 0)
            + pltpu.roll(w, 1, 0)
            + jnp.where(lane == height - 1, 0.0, pltpu.roll(s, height - 1, 1))
            + jnp.where(lane == 0, 0.0, pltpu.roll(n, 1, 1))
            for e, w, s, n in zip(from_east, from_west, from_south, from_north)
        ]
        state = [wet * update[0], damping * update[1], damping * update[2]]
    for c in range(3):
        last = (4 * c - 2) % LANES
        rows[last : last + 2] = state[c][KEEP - 2 : KEEP]
        rows[4 * c : 4 * c + 2] = state[c][SLOT - KEEP : SLOT - KEEP + 2]
    lane = lax.broadcasted_iota(jnp.int32, (LANES, LANES), 1)
    for block in range(height // LANES):
        span = slice(block * LANES, (block + 1) * LANES)
        turned_back = rows[:, span].T
        columns[span] = turned_back
        target, first = (top, 0) if block * LANES < width else (bottom, width)
        for end, chosen in ((0, lane < 2), (width - LANES, lane >= LANES - 2)):
            target[block * LANES - first : (block + 1) * LANES - first, end : end + LANES] = (
                jnp.where(chosen, turned_back, depth[span, end : end + LANES])
            )


def finish_kernel(
    top, bottom, columns, middle, damping, result, momenta, south, north, sent
):
    height, width = damping.shape
    copies = [
        pltpu.make_async_copy(top, result.at[0, 0:width], sent.at[0]),
        pltpu.make_async_copy(bottom, result.at[0, width:height], sent.at[1]),
    ]
    for copy in copies:
        copy.start()
    lane = lax.broadcasted_iota(jnp.int32, (SUBLANES, LANES), 1)
    tiles = width // LANES

    def store(group, t, update):
        span = tile_span(group, t)
        for i in range(2):
            value = damping[span] * update[i]
            if t == 0 or t == tiles - 1:
                outer = pltpu.roll(columns[rows_of(group), :], LANES - 4 * (i + 1), 1)
            if t == 0:
                value = jnp.where(lane < 2, outer, value)
            if t == tiles - 1:
                value = jnp.where(lane >= LANES - 2, outer, value)
            momenta[(i, *span)] = value

    sweep(height, width, (1, 2), FEW, partial(load_state, middle), store, south, north)
    copies.append(pltpu.make_async_copy(momenta, result.at[1:3], sent.at[2]))
    copies[-1].start()
    for copy in copies:
        copy.wait()


def place_kernel(top, bottom, result, sent):
    side = top.shape[0]
    copies = [
        pltpu.make_async_copy(top, result.at[0:side], sent.at[0]),
        pltpu.make_async_copy(bottom, result.at[side : 2 * side], sent.at[1]),
    ]
    for copy in copies:
        copy.start()
    for copy in copies:
        copy.wait()


def direct(top, bottom, columns, middle, damping, first, second):
    _, height, width = middle.shape
    f32 = jnp.float32

    def move(tile, distance):
        if distance == 0:
            return tile
        count = lax.axis_size("gx")
        return lax.ppermute(tile, "gx", [(i, i ^ distance) for i in range(count)])

    moved = move(top, first), move(bottom, second)
    final_fields = pl.pallas_call(
        finish_kernel,
        out_shape=pltpu.HBM(middle.shape, f32),
        in_specs=[VMEM] * 5,
        out_specs=HBM,
        scratch_shapes=[
            pltpu.VMEM((2, height, width), f32),
            pltpu.VMEM((2, width // LANES, height + SUBLANES, LANES), f32),
            pltpu.VMEM((2, width // LANES, height + SUBLANES, LANES), f32),
            pltpu.SemaphoreType.DMA((3,)),
        ],
        compiler_params=PARAMS,
        cost_estimate=pl.CostEstimate(
            flops=100 * middle.size, bytes_accessed=8 * middle.size, transcendentals=0
        ),
        name="finish",
    )(top, bottom, columns, middle, damping)
    owned_depth = pl.pallas_call(
        place_kernel,
        out_shape=pltpu.HBM((height, width), f32),
        in_specs=[VMEM] * 2,
        out_specs=HBM,
        scratch_shapes=[pltpu.SemaphoreType.DMA((2,))],
        compiler_params=PARAMS,
        name="place",
    )(*moved)
    return final_fields, owned_depth


def in_hbm(x):
    return pltpu.with_memory_space_constraint(x, pltpu.HBM)


def body(fields, friction, wet_mask, owner_table):
    _, height, width = fields.shape
    count = lax.axis_size("gx")
    distances = 1 << LEVELS
    blocks = height // LANES
    f32 = jnp.float32
    row_payload = jax.ShapeDtypeStruct((SUBLANES, height), f32)
    fields, friction, wet_mask, turned, pay_pair, pay_other, choice = pl.pallas_call(
        pack_kernel,
        out_shape=[
            jax.ShapeDtypeStruct(fields.shape, f32),
            jax.ShapeDtypeStruct(friction.shape, f32),
            jax.ShapeDtypeStruct(wet_mask.shape, jnp.int32),
            jax.ShapeDtypeStruct((4 * SUBLANES, height), f32),
            row_payload,
            row_payload,
            pltpu.HBM((1,), jnp.int32),
        ],
        in_specs=[HBM] * 4,
        out_specs=[VMEM] * 6 + [HBM],
        scratch_shapes=[
            pltpu.SMEM(owner_table.shape, jnp.int32),
            pltpu.SMEM((1,), jnp.int32),
            pltpu.SemaphoreType.DMA((blocks, 3)),
            pltpu.SemaphoreType.DMA,
        ],
        compiler_params=PARAMS,
        name="pack",
    )(*[in_hbm(x) for x in (fields, friction, wet_mask, owner_table)])
    got_pair = lax.ppermute(pay_pair, "gx", [(i, i ^ 1) for i in range(count)])
    others = [(i, i + 1) for i in range(1, count - 1, 2)]
    got_other = lax.ppermute(pay_other, "gx", others + [(b, a) for a, b in others])
    stripe = jax.ShapeDtypeStruct((height, width), f32)
    depth, middle, damping = pl.pallas_call(
        main_kernel,
        out_shape=[stripe, jax.ShapeDtypeStruct(fields.shape, f32), stripe],
        in_specs=[VMEM] * 3,
        out_specs=[VMEM] * 3,
        scratch_shapes=[
            pltpu.VMEM((height, width), f32),
            pltpu.VMEM((3, width // LANES, height + SUBLANES, LANES), f32),
            pltpu.VMEM((3, width // LANES, height + SUBLANES, LANES), f32),
        ],
        compiler_params=PARAMS,
        cost_estimate=pl.CostEstimate(
            flops=200 * fields.size, bytes_accessed=16 * height * width, transcendentals=0
        ),
        name="step",
    )(fields, friction, wet_mask)
    tile = jax.ShapeDtypeStruct((width, width), f32)
    top, bottom, columns = pl.pallas_call(
        edge_kernel,
        out_shape=[tile, tile, jax.ShapeDtypeStruct((height, LANES), f32)],
        in_specs=[VMEM] * 4,
        out_specs=[VMEM] * 3,
        scratch_shapes=[pltpu.VMEM((LANES, height), f32)],
        compiler_params=PARAMS,
        name="edge_columns",
    )(turned, got_pair, got_other, depth)
    return lax.switch(
        choice[0],
        [
            partial(direct, first=first, second=second)
            for first in range(distances)
            for second in range(distances)
        ],
        top,
        bottom,
        columns,
        middle,
        damping,
    )


def solution(mesh):
    in_specs = (P(None, "groups", "gx"), P("groups", "gx"), P("groups", "gx"), P("groups", None))
    out_specs = (P(None, "groups", "gx"), P("groups", "gx"))
    return jax.shard_map(body, mesh=mesh, in_specs=in_specs, out_specs=out_specs, check_vma=False)
```

```python
from functools import partial

import jax
import jax.numpy as jnp
from jax import lax
from jax.experimental import pallas as pl
from jax.experimental.pallas import tpu as pltpu
from jax.sharding import PartitionSpec as P

STEPS = 2
LEVELS = 3
LANES = 128
SUBLANES = 8
UNROLL = 16
FEW = 4
SLOT = 16
KEEP = 4
VMEM_BYTES = 16 * 1024 * 1024

depth_floor = 0.25
flux_factor = 0.1
time_step = 0.25

VMEM = pl.BlockSpec(memory_space=pltpu.VMEM)
HBM = pl.BlockSpec(memory_space=pltpu.HBM)
PARAMS = pltpu.CompilerParams(vmem_limit_bytes=VMEM_BYTES)


def flux_terms(depth, east, south):
    inverse = flux_factor / jnp.maximum(depth, depth_floor)
    speed_east = inverse * east
    speed_south = inverse * south
    pressure = (0.5 * flux_factor) * depth * depth
    cross = south * speed_east
    flux_east = (flux_factor * east, east * speed_east + pressure, cross)
    flux_south = (flux_factor * south, cross, south * speed_south + pressure)
    quarter = (0.25 * depth, 0.25 * east, 0.25 * south)
    from_east = [a - f for a, f in zip(quarter, flux_east)]
    from_west = [a + f for a, f in zip(quarter, flux_east)]
    from_south = [a - g for a, g in zip(quarter, flux_south)]
    from_north = [a + g for a, g in zip(quarter, flux_south)]
    return from_east, from_west, from_south, from_north


def pack_kernel(
    fields_in, friction_in, mask_in, table_in,
    fields, friction, wet_mask, turned, pay_pair, pay_other, choice,
    table, key_cell, arrived, told,
):
    height, width = fields.shape[1], fields.shape[2]
    count = height // LANES
    read_table = pltpu.make_async_copy(table_in, table, told)
    read_table.start()
    copies = []
    for block in range(count):
        span = pl.ds(block * LANES, LANES)
        copies.append(
            [
                pltpu.make_async_copy(fields_in.at[:, span], fields.at[:, span], arrived.at[block, 0]),
                pltpu.make_async_copy(friction_in.at[span], friction.at[span], arrived.at[block, 1]),
                pltpu.make_async_copy(mask_in.at[span], wet_mask.at[span], arrived.at[block, 2]),
            ]
        )
        for copy in copies[-1]:
            copy.start()
    read_table.wait()
    column = lax.axis_index("gx")
    key = 0
    for tile_row in range(table.shape[0]):
        key = (key << LEVELS) + (table[tile_row, column] ^ column)
    key_cell[0] = key
    write_key = pltpu.make_async_copy(key_cell, choice, told)
    write_key.start()
    lane = lax.broadcasted_iota(jnp.int32, (LANES, LANES), 1)
    ends = (slice(0, LANES), slice(width - LANES, width))

    def outer(left, right):
        return jnp.where(lane < KEEP, left, right)

    for block in range(count):
        for copy in copies[block]:
            copy.wait()
        span = slice(block * LANES, (block + 1) * LANES)
        openness = outer(
            *[wet_mask[span, end].astype(jnp.float32) * friction[span, end] for end in ends]
        )
        wet = (openness > 0.0).astype(jnp.float32)
        packed = openness
        for c in range(3):
            value = outer(*[fields[c, span, end] for end in ends]) * wet
            value = pltpu.roll(value, (c - 3) * SUBLANES % LANES, 1)
            start = (c - 3) * SUBLANES - KEEP + LANES
            packed = jnp.where((lane >= start) & (lane < start + SUBLANES), value, packed)
        packed = pltpu.roll(packed, 3 * SUBLANES + KEEP, 1)
        turned[:, span] = packed.T[0 : 4 * SUBLANES]
    even = lax.rem(lax.axis_index("gx"), 2) == 0
    for index in range(4):
        for far in range(2):
            right = turned[pl.ds(index * SUBLANES + KEEP - 1 - far, 1), :]
            left = turned[pl.ds(index * SUBLANES + KEEP + far, 1), :]
            pay_pair[pl.ds(4 * far + index, 1), :] = jnp.where(even, right, left)
            pay_other[pl.ds(4 * far + index, 1), :] = jnp.where(even, left, right)
    write_key.wait()


def rows_of(group, offset=0):
    start = group * SUBLANES
    if not isinstance(start, int):
        start = pl.multiple_of(start, SUBLANES)
    return pl.ds(start + offset, SUBLANES)


def sweep(height, width, parts, unroll, load, store, south, north):
    groups = height // SUBLANES
    tiles = width // LANES
    lane = lax.broadcasted_iota(jnp.int32, (SUBLANES, LANES), 1)
    first_lane, last_lane = lane == 0, lane == LANES - 1
    zero = jnp.zeros((SUBLANES, LANES), jnp.float32)
    for i in range(len(parts)):
        for t in range(tiles):
            north[i, t, 0:SUBLANES] = zero
            south[i, t, height : height + SUBLANES] = zero

    def across(from_east, from_west):
        east = [pltpu.roll(x, LANES - 1, 1) for x in from_east]
        west = [pltpu.roll(x, 1, 1) for x in from_west]
        return [
            jnp.where(last_lane, east[(t + 1) % tiles], east[t])
            + jnp.where(first_lane, west[t - 1], west[t])
            for t in range(tiles)
        ]

    def finish(group, held):
        for t in range(tiles):
            below = [south[i, t, rows_of(group, 1)] for i in range(len(parts))]
            store(group, t, [held[i][t] + below[i] for i in range(len(parts))])

    def one(group, held):
        per_tile = [flux_terms(*state) for state in load(group)]
        for t in range(tiles):
            for i, part in enumerate(parts):
                south[i, t, rows_of(group)] = per_tile[t][2][part]
                north[i, t, rows_of(group + 1)] = per_tile[t][3][part]
        finish(jnp.maximum(group - 1, 0), held)
        held = []
        for i, part in enumerate(parts):
            side = across([x[0][part] for x in per_tile], [x[1][part] for x in per_tile])
            held.append([side[t] + north[i, t, rows_of(group, SUBLANES - 1)] for t in range(tiles)])
        return held

    def trip(k, held):
        for j in range(unroll):
            held = one(k * unroll + j, held)
        return held

    held = lax.fori_loop(0, groups // unroll, trip, [[zero] * tiles] * len(parts))
    finish(groups - 1, held)


def tile_span(group, t):
    return (rows_of(group), slice(t * LANES, (t + 1) * LANES))


def load_state(middle, group):
    tiles = middle.shape[2] // LANES
    return [[middle[(c, *tile_span(group, t))] for c in range(3)] for t in range(tiles)]


def main_kernel(fields, friction, wet_mask, depth, middle, damping, wet_cells, south, north):
    height, width = depth.shape
    tiles = width // LANES

    def load(group):
        states = []
        for t in range(tiles):
            span = tile_span(group, t)
            openness = wet_mask[span].astype(jnp.float32) * friction[span]
            wet = (openness > 0.0).astype(jnp.float32)
            wet_cells[span] = wet
            damping[span] = wet / (1.0 + time_step * openness)
            states.append([fields[(c, *span)] * wet for c in range(3)])
        return states

    def store(group, t, update):
        span = tile_span(group, t)
        damp = damping[span]
        middle[(0, *span)] = wet_cells[span] * update[0]
        middle[(1, *span)] = damp * update[1]
        middle[(2, *span)] = damp * update[2]

    def store_depth(group, t, update):
        span = tile_span(group, t)
        depth[span] = wet_cells[span] * update[0]

    sweep(height, width, (0, 1, 2), UNROLL, load, store, south, north)
    sweep(height, width, (0,), UNROLL, partial(load_state, middle), store_depth, south, north)


def edge_kernel(turned, got_pair, got_other, depth, top, bottom, columns, rows):
    height, width = depth.shape
    rows[...] = jnp.zeros_like(rows)
    column = lax.axis_index("gx")
    even = lax.rem(column, 2) == 0
    outside = (column == 0) | (column == lax.axis_size("gx") - 1)
    for index in range(4):
        start = index * SLOT
        own = index * SUBLANES
        rows[start : start + KEEP] = turned[own : own + KEEP]
        rows[start + SLOT - KEEP : start + SLOT] = turned[own + KEEP : own + 2 * KEEP]
        for far in range(2):
            pair = got_pair[pl.ds(4 * far + index, 1), :]
            other = jnp.where(outside, 0.0, got_other[pl.ds(4 * far + index, 1), :])
            rows[pl.ds(start + SLOT - KEEP - 1 - far, 1), :] = jnp.where(even, other, pair)
            rows[pl.ds(start + KEEP + far, 1), :] = jnp.where(even, pair, other)
    lane = lax.broadcasted_iota(jnp.int32, (SLOT, height), 1)
    state = [rows[c * SLOT : (c + 1) * SLOT] for c in range(3)]
    openness = rows[3 * SLOT : 4 * SLOT]
    wet = (openness > 0.0).astype(jnp.float32)
    damping = wet / (1.0 + time_step * openness)
    for _ in range(STEPS):
        from_east, from_west, from_south, from_north = flux_terms(*state)
        update = [
            pltpu.roll(e, SLOT - 1, 0)
            + pltpu.roll(w, 1, 0)
            + jnp.where(lane == height - 1, 0.0, pltpu.roll(s, height - 1, 1))
            + jnp.where(lane == 0, 0.0, pltpu.roll(n, 1, 1))
            for e, w, s, n in zip(from_east, from_west, from_south, from_north)
        ]
        state = [wet * update[0], damping * update[1], damping * update[2]]
    for c in range(3):
        last = (4 * c - 2) % LANES
        rows[last : last + 2] = state[c][KEEP - 2 : KEEP]
        rows[4 * c : 4 * c + 2] = state[c][SLOT - KEEP : SLOT - KEEP + 2]
    lane = lax.broadcasted_iota(jnp.int32, (LANES, LANES), 1)
    for block in range(height // LANES):
        span = slice(block * LANES, (block + 1) * LANES)
        turned_back = rows[:, span].T
        columns[span] = turned_back
        target, first = (top, 0) if block * LANES < width else (bottom, width)
        for end, chosen in ((0, lane < 2), (width - LANES, lane >= LANES - 2)):
            target[block * LANES - first : (block + 1) * LANES - first, end : end + LANES] = (
                jnp.where(chosen, turned_back, depth[span, end : end + LANES])
            )


def finish_kernel(
    top, bottom, columns, middle, damping, result, momenta, south, north, sent
):
    height, width = damping.shape
    copies = [
        pltpu.make_async_copy(top, result.at[0, 0:width], sent.at[0]),
        pltpu.make_async_copy(bottom, result.at[0, width:height], sent.at[1]),
    ]
    for copy in copies:
        copy.start()
    lane = lax.broadcasted_iota(jnp.int32, (SUBLANES, LANES), 1)
    tiles = width // LANES

    def store(group, t, update):
        span = tile_span(group, t)
        for i in range(2):
            value = damping[span] * update[i]
            if t == 0 or t == tiles - 1:
                outer = pltpu.roll(columns[rows_of(group), :], LANES - 4 * (i + 1), 1)
            if t == 0:
                value = jnp.where(lane < 2, outer, value)
            if t == tiles - 1:
                value = jnp.where(lane >= LANES - 2, outer, value)
            momenta[(i, *span)] = value

    sweep(height, width, (1, 2), FEW, partial(load_state, middle), store, south, north)
    copies.append(pltpu.make_async_copy(momenta, result.at[1:3], sent.at[2]))
    copies[-1].start()
    for copy in copies:
        copy.wait()


def place_kernel(top, bottom, result, sent):
    side = top.shape[0]
    copies = [
        pltpu.make_async_copy(top, result.at[0:side], sent.at[0]),
        pltpu.make_async_copy(bottom, result.at[side : 2 * side], sent.at[1]),
    ]
    for copy in copies:
        copy.start()
    for copy in copies:
        copy.wait()


def direct(top, bottom, columns, middle, damping, first, second):
    _, height, width = middle.shape
    f32 = jnp.float32

    def move(tile, distance):
        if distance == 0:
            return tile
        count = lax.axis_size("gx")
        return lax.ppermute(tile, "gx", [(i, i ^ distance) for i in range(count)])

    moved = move(top, first), move(bottom, second)
    final_fields = pl.pallas_call(
        finish_kernel,
        out_shape=pltpu.HBM(middle.shape, f32),
        in_specs=[VMEM] * 5,
        out_specs=HBM,
        scratch_shapes=[
            pltpu.VMEM((2, height, width), f32),
            pltpu.VMEM((2, width // LANES, height + SUBLANES, LANES), f32),
            pltpu.VMEM((2, width // LANES, height + SUBLANES, LANES), f32),
            pltpu.SemaphoreType.DMA((3,)),
        ],
        compiler_params=PARAMS,
        cost_estimate=pl.CostEstimate(
            flops=100 * middle.size, bytes_accessed=8 * middle.size, transcendentals=0
        ),
        name="finish",
    )(top, bottom, columns, middle, damping)
    owned_depth = pl.pallas_call(
        place_kernel,
        out_shape=pltpu.HBM((height, width), f32),
        in_specs=[VMEM] * 2,
        out_specs=HBM,
        scratch_shapes=[pltpu.SemaphoreType.DMA((2,))],
        compiler_params=PARAMS,
        name="place",
    )(*moved)
    return final_fields, owned_depth


def other_pairs(count):
    groups = lax.axis_size("groups")
    pairs = []
    for group in range(groups):
        base = group * count
        pairs += [(base + i, base + i + 1) for i in range(1, count - 1, 2)]
        if groups % 2:
            pairs.append((base, base + count - 1))
        elif group % 2 == 0:
            pairs += [(base + end, base + count + end) for end in (0, count - 1)]
    return pairs + [(b, a) for a, b in pairs]


def in_hbm(x):
    return pltpu.with_memory_space_constraint(x, pltpu.HBM)


def body(fields, friction, wet_mask, owner_table):
    _, height, width = fields.shape
    count = lax.axis_size("gx")
    distances = 1 << LEVELS
    blocks = height // LANES
    f32 = jnp.float32
    row_payload = jax.ShapeDtypeStruct((SUBLANES, height), f32)
    fields, friction, wet_mask, turned, pay_pair, pay_other, choice = pl.pallas_call(
        pack_kernel,
        out_shape=[
            jax.ShapeDtypeStruct(fields.shape, f32),
            jax.ShapeDtypeStruct(friction.shape, f32),
            jax.ShapeDtypeStruct(wet_mask.shape, jnp.int32),
            jax.ShapeDtypeStruct((4 * SUBLANES, height), f32),
            row_payload,
            row_payload,
            pltpu.HBM((1,), jnp.int32),
        ],
        in_specs=[HBM] * 4,
        out_specs=[VMEM] * 6 + [HBM],
        scratch_shapes=[
            pltpu.SMEM(owner_table.shape, jnp.int32),
            pltpu.SMEM((1,), jnp.int32),
            pltpu.SemaphoreType.DMA((blocks, 3)),
            pltpu.SemaphoreType.DMA,
        ],
        compiler_params=PARAMS,
        name="pack",
    )(*[in_hbm(x) for x in (fields, friction, wet_mask, owner_table)])
    got_pair = lax.ppermute(pay_pair, "gx", [(i, i ^ 1) for i in range(count)])
    got_other = lax.ppermute(pay_other, ("groups", "gx"), other_pairs(count))
    stripe = jax.ShapeDtypeStruct((height, width), f32)
    depth, middle, damping = pl.pallas_call(
        main_kernel,
        out_shape=[stripe, jax.ShapeDtypeStruct(fields.shape, f32), stripe],
        in_specs=[VMEM] * 3,
        out_specs=[VMEM] * 3,
        scratch_shapes=[
            pltpu.VMEM((height, width), f32),
            pltpu.VMEM((3, width // LANES, height + SUBLANES, LANES), f32),
            pltpu.VMEM((3, width // LANES, height + SUBLANES, LANES), f32),
        ],
        compiler_params=PARAMS,
        cost_estimate=pl.CostEstimate(
            flops=200 * fields.size, bytes_accessed=16 * height * width, transcendentals=0
        ),
        name="step",
    )(fields, friction, wet_mask)
    tile = jax.ShapeDtypeStruct((width, width), f32)
    top, bottom, columns = pl.pallas_call(
        edge_kernel,
        out_shape=[tile, tile, jax.ShapeDtypeStruct((height, LANES), f32)],
        in_specs=[VMEM] * 4,
        out_specs=[VMEM] * 3,
        scratch_shapes=[pltpu.VMEM((LANES, height), f32)],
        compiler_params=PARAMS,
        name="edge_columns",
    )(turned, got_pair, got_other, depth)
    return lax.switch(
        choice[0],
        [
            partial(direct, first=first, second=second)
            for first in range(distances)
            for second in range(distances)
        ],
        top,
        bottom,
        columns,
        middle,
        damping,
    )


def solution(mesh):
    in_specs = (P(None, "groups", "gx"), P("groups", "gx"), P("groups", "gx"), P("groups", None))
    out_specs = (P(None, "groups", "gx"), P("groups", "gx"))
    return jax.shard_map(body, mesh=mesh, in_specs=in_specs, out_specs=out_specs, check_vma=False)
```

```python
from functools import partial

import jax
import jax.numpy as jnp
from jax import lax
from jax.experimental import pallas as pl
from jax.experimental.pallas import tpu as pltpu
from jax.sharding import PartitionSpec as P

STEPS = 2
LEVELS = 3
LANES = 128
SUBLANES = 8
UNROLL = 16
FEW = 4
SLOT = 16
KEEP = 4
VMEM_BYTES = 16 * 1024 * 1024

depth_floor = 0.25
flux_factor = 0.1
time_step = 0.25

VMEM = pl.BlockSpec(memory_space=pltpu.VMEM)
HBM = pl.BlockSpec(memory_space=pltpu.HBM)
SMEM = pl.BlockSpec(memory_space=pltpu.SMEM)
PARAMS = pltpu.CompilerParams(vmem_limit_bytes=VMEM_BYTES)


def flux_terms(depth, east, south):
    inverse = flux_factor / jnp.maximum(depth, depth_floor)
    speed_east = inverse * east
    speed_south = inverse * south
    pressure = (0.5 * flux_factor) * depth * depth
    cross = south * speed_east
    flux_east = (flux_factor * east, east * speed_east + pressure, cross)
    flux_south = (flux_factor * south, cross, south * speed_south + pressure)
    quarter = (0.25 * depth, 0.25 * east, 0.25 * south)
    from_east = [a - f for a, f in zip(quarter, flux_east)]
    from_west = [a + f for a, f in zip(quarter, flux_east)]
    from_south = [a - g for a, g in zip(quarter, flux_south)]
    from_north = [a + g for a, g in zip(quarter, flux_south)]
    return from_east, from_west, from_south, from_north


def pack_kernel(
    fields_in, friction_in, mask_in, table_in,
    fields, friction, wet_mask, turned, pay_pair, pay_other, choice,
    table, arrived, told,
):
    height, width = fields.shape[1], fields.shape[2]
    count = height // LANES
    read_table = pltpu.make_async_copy(table_in, table, told)
    read_table.start()
    copies = []
    for block in range(count):
        span = pl.ds(block * LANES, LANES)
        copies.append(
            [
                pltpu.make_async_copy(fields_in.at[:, span], fields.at[:, span], arrived.at[block, 0]),
                pltpu.make_async_copy(friction_in.at[span], friction.at[span], arrived.at[block, 1]),
                pltpu.make_async_copy(mask_in.at[span], wet_mask.at[span], arrived.at[block, 2]),
            ]
        )
        for copy in copies[-1]:
            copy.start()
    read_table.wait()
    column = lax.axis_index("gx")
    key = 0
    for tile_row in range(table.shape[0]):
        key = (key << LEVELS) + (table[tile_row, column] ^ column)
    choice[0] = key
    lane = lax.broadcasted_iota(jnp.int32, (LANES, LANES), 1)
    ends = (slice(0, LANES), slice(width - LANES, width))

    def outer(left, right):
        return jnp.where(lane < KEEP, left, right)

    for block in range(count):
        for copy in copies[block]:
            copy.wait()
        span = slice(block * LANES, (block + 1) * LANES)
        openness = outer(
            *[wet_mask[span, end].astype(jnp.float32) * friction[span, end] for end in ends]
        )
        wet = (openness > 0.0).astype(jnp.float32)
        packed = openness
        for c in range(3):
            value = outer(*[fields[c, span, end] for end in ends]) * wet
            value = pltpu.roll(value, (c - 3) * SUBLANES % LANES, 1)
            start = (c - 3) * SUBLANES - KEEP + LANES
            packed = jnp.where((lane >= start) & (lane < start + SUBLANES), value, packed)
        packed = pltpu.roll(packed, 3 * SUBLANES + KEEP, 1)
        turned[:, span] = packed.T[0 : 4 * SUBLANES]
    even = lax.rem(lax.axis_index("gx"), 2) == 0
    for index in range(4):
        for far in range(2):
            right = turned[pl.ds(index * SUBLANES + KEEP - 1 - far, 1), :]
            left = turned[pl.ds(index * SUBLANES + KEEP + far, 1), :]
            pay_pair[pl.ds(4 * far + index, 1), :] = jnp.where(even, right, left)
            pay_other[pl.ds(4 * far + index, 1), :] = jnp.where(even, left, right)


def rows_of(group, offset=0):
    start = group * SUBLANES
    if not isinstance(start, int):
        start = pl.multiple_of(start, SUBLANES)
    return pl.ds(start + offset, SUBLANES)


def sweep(height, width, parts, unroll, load, store, south, north):
    groups = height // SUBLANES
    tiles = width // LANES
    lane = lax.broadcasted_iota(jnp.int32, (SUBLANES, LANES), 1)
    first_lane, last_lane = lane == 0, lane == LANES - 1
    zero = jnp.zeros((SUBLANES, LANES), jnp.float32)
    for i in range(len(parts)):
        for t in range(tiles):
            north[i, t, 0:SUBLANES] = zero
            south[i, t, height : height + SUBLANES] = zero

    def across(from_east, from_west):
        east = [pltpu.roll(x, LANES - 1, 1) for x in from_east]
        west = [pltpu.roll(x, 1, 1) for x in from_west]
        return [
            jnp.where(last_lane, east[(t + 1) % tiles], east[t])
            + jnp.where(first_lane, west[t - 1], west[t])
            for t in range(tiles)
        ]

    def finish(group, held):
        for t in range(tiles):
            below = [south[i, t, rows_of(group, 1)] for i in range(len(parts))]
            store(group, t, [held[i][t] + below[i] for i in range(len(parts))])

    def one(group, held):
        per_tile = [flux_terms(*state) for state in load(group)]
        for t in range(tiles):
            for i, part in enumerate(parts):
                south[i, t, rows_of(group)] = per_tile[t][2][part]
                north[i, t, rows_of(group + 1)] = per_tile[t][3][part]
        finish(jnp.maximum(group - 1, 0), held)
        held = []
        for i, part in enumerate(parts):
            side = across([x[0][part] for x in per_tile], [x[1][part] for x in per_tile])
            held.append([side[t] + north[i, t, rows_of(group, SUBLANES - 1)] for t in range(tiles)])
        return held

    def trip(k, held):
        for j in range(unroll):
            held = one(k * unroll + j, held)
        return held

    held = lax.fori_loop(0, groups // unroll, trip, [[zero] * tiles] * len(parts))
    finish(groups - 1, held)


def tile_span(group, t):
    return (rows_of(group), slice(t * LANES, (t + 1) * LANES))


def load_state(middle, group):
    tiles = middle.shape[2] // LANES
    return [[middle[(c, *tile_span(group, t))] for c in range(3)] for t in range(tiles)]


def main_kernel(fields, friction, wet_mask, depth, middle, damping, wet_cells, south, north):
    height, width = depth.shape
    tiles = width // LANES

    def load(group):
        states = []
        for t in range(tiles):
            span = tile_span(group, t)
            openness = wet_mask[span].astype(jnp.float32) * friction[span]
            wet = (openness > 0.0).astype(jnp.float32)
            wet_cells[span] = wet
            damping[span] = wet / (1.0 + time_step * openness)
            states.append([fields[(c, *span)] * wet for c in range(3)])
        return states

    def store(group, t, update):
        span = tile_span(group, t)
        damp = damping[span]
        middle[(0, *span)] = wet_cells[span] * update[0]
        middle[(1, *span)] = damp * update[1]
        middle[(2, *span)] = damp * update[2]

    def store_depth(group, t, update):
        span = tile_span(group, t)
        depth[span] = wet_cells[span] * update[0]

    sweep(height, width, (0, 1, 2), UNROLL, load, store, south, north)
    sweep(height, width, (0,), UNROLL, partial(load_state, middle), store_depth, south, north)


def edge_kernel(turned, got_pair, got_other, depth, top, bottom, columns, rows):
    height, width = depth.shape
    rows[...] = jnp.zeros_like(rows)
    column = lax.axis_index("gx")
    even = lax.rem(column, 2) == 0
    outside = (column == 0) | (column == lax.axis_size("gx") - 1)
    for index in range(4):
        start = index * SLOT
        own = index * SUBLANES
        rows[start : start + KEEP] = turned[own : own + KEEP]
        rows[start + SLOT - KEEP : start + SLOT] = turned[own + KEEP : own + 2 * KEEP]
        for far in range(2):
            pair = got_pair[pl.ds(4 * far + index, 1), :]
            other = jnp.where(outside, 0.0, got_other[pl.ds(4 * far + index, 1), :])
            rows[pl.ds(start + SLOT - KEEP - 1 - far, 1), :] = jnp.where(even, other, pair)
            rows[pl.ds(start + KEEP + far, 1), :] = jnp.where(even, pair, other)
    lane = lax.broadcasted_iota(jnp.int32, (SLOT, height), 1)
    state = [rows[c * SLOT : (c + 1) * SLOT] for c in range(3)]
    openness = rows[3 * SLOT : 4 * SLOT]
    wet = (openness > 0.0).astype(jnp.float32)
    damping = wet / (1.0 + time_step * openness)
    for _ in range(STEPS):
        from_east, from_west, from_south, from_north = flux_terms(*state)
        update = [
            pltpu.roll(e, SLOT - 1, 0)
            + pltpu.roll(w, 1, 0)
            + jnp.where(lane == height - 1, 0.0, pltpu.roll(s, height - 1, 1))
            + jnp.where(lane == 0, 0.0, pltpu.roll(n, 1, 1))
            for e, w, s, n in zip(from_east, from_west, from_south, from_north)
        ]
        state = [wet * update[0], damping * update[1], damping * update[2]]
    for c in range(3):
        last = (4 * c - 2) % LANES
        rows[last : last + 2] = state[c][KEEP - 2 : KEEP]
        rows[4 * c : 4 * c + 2] = state[c][SLOT - KEEP : SLOT - KEEP + 2]
    lane = lax.broadcasted_iota(jnp.int32, (LANES, LANES), 1)
    for block in range(height // LANES):
        span = slice(block * LANES, (block + 1) * LANES)
        turned_back = rows[:, span].T
        columns[span] = turned_back
        target, first = (top, 0) if block * LANES < width else (bottom, width)
        for end, chosen in ((0, lane < 2), (width - LANES, lane >= LANES - 2)):
            target[block * LANES - first : (block + 1) * LANES - first, end : end + LANES] = (
                jnp.where(chosen, turned_back, depth[span, end : end + LANES])
            )


def finish_kernel(
    top, bottom, columns, middle, damping, result, momenta, south, north, sent
):
    height, width = damping.shape
    copies = [
        pltpu.make_async_copy(top, result.at[0, 0:width], sent.at[0]),
        pltpu.make_async_copy(bottom, result.at[0, width:height], sent.at[1]),
    ]
    for copy in copies:
        copy.start()
    lane = lax.broadcasted_iota(jnp.int32, (SUBLANES, LANES), 1)
    tiles = width // LANES

    def store(group, t, update):
        span = tile_span(group, t)
        for i in range(2):
            value = damping[span] * update[i]
            if t == 0 or t == tiles - 1:
                outer = pltpu.roll(columns[rows_of(group), :], LANES - 4 * (i + 1), 1)
            if t == 0:
                value = jnp.where(lane < 2, outer, value)
            if t == tiles - 1:
                value = jnp.where(lane >= LANES - 2, outer, value)
            momenta[(i, *span)] = value

    sweep(height, width, (1, 2), FEW, partial(load_state, middle), store, south, north)
    copies.append(pltpu.make_async_copy(momenta, result.at[1:3], sent.at[2]))
    copies[-1].start()
    for copy in copies:
        copy.wait()


def place_kernel(top, bottom, result, sent):
    side = top.shape[0]
    copies = [
        pltpu.make_async_copy(top, result.at[0:side], sent.at[0]),
        pltpu.make_async_copy(bottom, result.at[side : 2 * side], sent.at[1]),
    ]
    for copy in copies:
        copy.start()
    for copy in copies:
        copy.wait()


def direct(top, bottom, columns, middle, damping, first, second):
    _, height, width = middle.shape
    f32 = jnp.float32

    def move(tile, distance):
        if distance == 0:
            return tile
        count = lax.axis_size("gx")
        return lax.ppermute(tile, "gx", [(i, i ^ distance) for i in range(count)])

    moved = move(top, first), move(bottom, second)
    final_fields = pl.pallas_call(
        finish_kernel,
        out_shape=pltpu.HBM(middle.shape, f32),
        in_specs=[VMEM] * 5,
        out_specs=HBM,
        scratch_shapes=[
            pltpu.VMEM((2, height, width), f32),
            pltpu.VMEM((2, width // LANES, height + SUBLANES, LANES), f32),
            pltpu.VMEM((2, width // LANES, height + SUBLANES, LANES), f32),
            pltpu.SemaphoreType.DMA((3,)),
        ],
        compiler_params=PARAMS,
        cost_estimate=pl.CostEstimate(
            flops=100 * middle.size, bytes_accessed=8 * middle.size, transcendentals=0
        ),
        name="finish",
    )(top, bottom, columns, middle, damping)
    owned_depth = pl.pallas_call(
        place_kernel,
        out_shape=pltpu.HBM((height, width), f32),
        in_specs=[VMEM] * 2,
        out_specs=HBM,
        scratch_shapes=[pltpu.SemaphoreType.DMA((2,))],
        compiler_params=PARAMS,
        name="place",
    )(*moved)
    return final_fields, owned_depth


def other_pairs(count):
    groups = lax.axis_size("groups")
    pairs = []
    for group in range(groups):
        base = group * count
        pairs += [(base + i, base + i + 1) for i in range(1, count - 1, 2)]
        if groups % 2:
            pairs.append((base, base + count - 1))
        elif group % 2 == 0:
            pairs += [(base + end, base + count + end) for end in (0, count - 1)]
    return pairs + [(b, a) for a, b in pairs]


def in_hbm(x):
    return pltpu.with_memory_space_constraint(x, pltpu.HBM)


def body(fields, friction, wet_mask, owner_table):
    _, height, width = fields.shape
    count = lax.axis_size("gx")
    distances = 1 << LEVELS
    blocks = height // LANES
    f32 = jnp.float32
    row_payload = jax.ShapeDtypeStruct((SUBLANES, height), f32)
    fields, friction, wet_mask, turned, pay_pair, pay_other, choice = pl.pallas_call(
        pack_kernel,
        out_shape=[
            jax.ShapeDtypeStruct(fields.shape, f32),
            jax.ShapeDtypeStruct(friction.shape, f32),
            jax.ShapeDtypeStruct(wet_mask.shape, jnp.int32),
            jax.ShapeDtypeStruct((4 * SUBLANES, height), f32),
            row_payload,
            row_payload,
            pltpu.SMEM((1,), jnp.int32),
        ],
        in_specs=[HBM] * 4,
        out_specs=[VMEM] * 6 + [SMEM],
        scratch_shapes=[
            pltpu.SMEM(owner_table.shape, jnp.int32),
            pltpu.SemaphoreType.DMA((blocks, 3)),
            pltpu.SemaphoreType.DMA,
        ],
        compiler_params=PARAMS,
        name="pack",
    )(*[in_hbm(x) for x in (fields, friction, wet_mask, owner_table)])
    got_pair = lax.ppermute(pay_pair, "gx", [(i, i ^ 1) for i in range(count)])
    got_other = lax.ppermute(pay_other, ("groups", "gx"), other_pairs(count))
    stripe = jax.ShapeDtypeStruct((height, width), f32)
    depth, middle, damping = pl.pallas_call(
        main_kernel,
        out_shape=[stripe, jax.ShapeDtypeStruct(fields.shape, f32), stripe],
        in_specs=[VMEM] * 3,
        out_specs=[VMEM] * 3,
        scratch_shapes=[
            pltpu.VMEM((height, width), f32),
            pltpu.VMEM((3, width // LANES, height + SUBLANES, LANES), f32),
            pltpu.VMEM((3, width // LANES, height + SUBLANES, LANES), f32),
        ],
        compiler_params=PARAMS,
        cost_estimate=pl.CostEstimate(
            flops=200 * fields.size, bytes_accessed=16 * height * width, transcendentals=0
        ),
        name="step",
    )(fields, friction, wet_mask)
    tile = jax.ShapeDtypeStruct((width, width), f32)
    top, bottom, columns = pl.pallas_call(
        edge_kernel,
        out_shape=[tile, tile, jax.ShapeDtypeStruct((height, LANES), f32)],
        in_specs=[VMEM] * 4,
        out_specs=[VMEM] * 3,
        scratch_shapes=[pltpu.VMEM((LANES, height), f32)],
        compiler_params=PARAMS,
        name="edge_columns",
    )(turned, got_pair, got_other, depth)
    return lax.switch(
        choice[0],
        [
            partial(direct, first=first, second=second)
            for first in range(distances)
            for second in range(distances)
        ],
        top,
        bottom,
        columns,
        middle,
        damping,
    )


def solution(mesh):
    in_specs = (P(None, "groups", "gx"), P("groups", "gx"), P("groups", "gx"), P("groups", None))
    out_specs = (P(None, "groups", "gx"), P("groups", "gx"))
    return jax.shard_map(body, mesh=mesh, in_specs=in_specs, out_specs=out_specs, check_vma=False)
```

```python
from functools import partial

import jax
import jax.numpy as jnp
from jax import lax
from jax.experimental import pallas as pl
from jax.experimental.pallas import tpu as pltpu
from jax.sharding import PartitionSpec as P

STEPS = 2
LEVELS = 3
LANES = 128
SUBLANES = 8
UNROLL = 16
FEW = 4
SLOT = 16
KEEP = 4
VMEM_BYTES = 16 * 1024 * 1024

depth_floor = 0.25
flux_factor = 0.1
time_step = 0.25

VMEM = pl.BlockSpec(memory_space=pltpu.VMEM)
HBM = pl.BlockSpec(memory_space=pltpu.HBM)
SMEM = pl.BlockSpec(memory_space=pltpu.SMEM)
PARAMS = pltpu.CompilerParams(vmem_limit_bytes=VMEM_BYTES)


def flux_terms(depth, east, south):
    inverse = flux_factor / jnp.maximum(depth, depth_floor)
    speed_east = inverse * east
    speed_south = inverse * south
    pressure = (0.5 * flux_factor) * depth * depth
    cross = south * speed_east
    flux_east = (flux_factor * east, east * speed_east + pressure, cross)
    flux_south = (flux_factor * south, cross, south * speed_south + pressure)
    quarter = (0.25 * depth, 0.25 * east, 0.25 * south)
    from_east = [a - f for a, f in zip(quarter, flux_east)]
    from_west = [a + f for a, f in zip(quarter, flux_east)]
    from_south = [a - g for a, g in zip(quarter, flux_south)]
    from_north = [a + g for a, g in zip(quarter, flux_south)]
    return from_east, from_west, from_south, from_north


def pack_kernel(
    fields_in, friction_in, mask_in, table_in,
    fields, friction, wet_mask, turned, pay_pair, pay_other, choice,
    table, arrived, told,
):
    height, width = fields.shape[1], fields.shape[2]
    count = height // LANES
    read_table = pltpu.make_async_copy(table_in, table, told)
    read_table.start()
    copies = []
    for block in range(count):
        span = pl.ds(block * LANES, LANES)
        copies.append(
            [
                pltpu.make_async_copy(fields_in.at[:, span], fields.at[:, span], arrived.at[block, 0]),
                pltpu.make_async_copy(friction_in.at[span], friction.at[span], arrived.at[block, 1]),
                pltpu.make_async_copy(mask_in.at[span], wet_mask.at[span], arrived.at[block, 2]),
            ]
        )
        for copy in copies[-1]:
            copy.start()
    read_table.wait()
    column = lax.axis_index("gx")
    key = 0
    for tile_row in range(table.shape[0]):
        key = (key << LEVELS) + (table[tile_row, column] ^ column)
    choice[0] = key
    lane = lax.broadcasted_iota(jnp.int32, (LANES, LANES), 1)
    ends = (slice(0, LANES), slice(width - LANES, width))

    def outer(left, right):
        return jnp.where(lane < KEEP, left, right)

    for block in range(count):
        for copy in copies[block]:
            copy.wait()
        span = slice(block * LANES, (block + 1) * LANES)
        openness = outer(
            *[wet_mask[span, end].astype(jnp.float32) * friction[span, end] for end in ends]
        )
        wet = (openness > 0.0).astype(jnp.float32)
        packed = openness
        for c in range(3):
            value = outer(*[fields[c, span, end] for end in ends]) * wet
            value = pltpu.roll(value, (c - 3) * SUBLANES % LANES, 1)
            start = (c - 3) * SUBLANES - KEEP + LANES
            packed = jnp.where((lane >= start) & (lane < start + SUBLANES), value, packed)
        packed = pltpu.roll(packed, 3 * SUBLANES + KEEP, 1)
        turned[:, span] = packed.T[0 : 4 * SUBLANES]
    even = lax.rem(lax.axis_index("gx"), 2) == 0
    for index in range(4):
        for far in range(2):
            right = turned[pl.ds(index * SUBLANES + KEEP - 1 - far, 1), :]
            left = turned[pl.ds(index * SUBLANES + KEEP + far, 1), :]
            pay_pair[pl.ds(4 * far + index, 1), :] = jnp.where(even, right, left)
            pay_other[pl.ds(4 * far + index, 1), :] = jnp.where(even, left, right)


def rows_of(group, offset=0):
    start = group * SUBLANES
    if not isinstance(start, int):
        start = pl.multiple_of(start, SUBLANES)
    return pl.ds(start + offset, SUBLANES)


def sweep(height, width, parts, unroll, load, store, south, north):
    groups = height // SUBLANES
    tiles = width // LANES
    lane = lax.broadcasted_iota(jnp.int32, (SUBLANES, LANES), 1)
    first_lane, last_lane = lane == 0, lane == LANES - 1
    zero = jnp.zeros((SUBLANES, LANES), jnp.float32)
    for i in range(len(parts)):
        for t in range(tiles):
            north[i, t, 0:SUBLANES] = zero
            south[i, t, height : height + SUBLANES] = zero

    def across(from_east, from_west):
        east = [pltpu.roll(x, LANES - 1, 1) for x in from_east]
        west = [pltpu.roll(x, 1, 1) for x in from_west]
        return [
            jnp.where(last_lane, east[(t + 1) % tiles], east[t])
            + jnp.where(first_lane, west[t - 1], west[t])
            for t in range(tiles)
        ]

    def finish(group, held):
        for t in range(tiles):
            below = [south[i, t, rows_of(group, 1)] for i in range(len(parts))]
            store(group, t, [held[i][t] + below[i] for i in range(len(parts))])

    def one(group, held):
        per_tile = [flux_terms(*state) for state in load(group)]
        for t in range(tiles):
            for i, part in enumerate(parts):
                south[i, t, rows_of(group)] = per_tile[t][2][part]
                north[i, t, rows_of(group + 1)] = per_tile[t][3][part]
        finish(jnp.maximum(group - 1, 0), held)
        held = []
        for i, part in enumerate(parts):
            side = across([x[0][part] for x in per_tile], [x[1][part] for x in per_tile])
            held.append([side[t] + north[i, t, rows_of(group, SUBLANES - 1)] for t in range(tiles)])
        return held

    def trip(k, held):
        for j in range(unroll):
            held = one(k * unroll + j, held)
        return held

    held = lax.fori_loop(0, groups // unroll, trip, [[zero] * tiles] * len(parts))
    finish(groups - 1, held)


def tile_span(group, t):
    return (rows_of(group), slice(t * LANES, (t + 1) * LANES))


def load_state(middle, group):
    tiles = middle.shape[2] // LANES
    return [[middle[(c, *tile_span(group, t))] for c in range(3)] for t in range(tiles)]


def main_kernel(fields, friction, wet_mask, depth, middle, damping, wet_cells, south, north):
    height, width = depth.shape
    tiles = width // LANES

    def load(group):
        states = []
        for t in range(tiles):
            span = tile_span(group, t)
            openness = wet_mask[span].astype(jnp.float32) * friction[span]
            wet = (openness > 0.0).astype(jnp.float32)
            wet_cells[span] = wet
            damping[span] = wet / (1.0 + time_step * openness)
            states.append([fields[(c, *span)] * wet for c in range(3)])
        return states

    def store(group, t, update):
        span = tile_span(group, t)
        damp = damping[span]
        middle[(0, *span)] = wet_cells[span] * update[0]
        middle[(1, *span)] = damp * update[1]
        middle[(2, *span)] = damp * update[2]

    def store_depth(group, t, update):
        span = tile_span(group, t)
        depth[span] = wet_cells[span] * update[0]

    sweep(height, width, (0, 1, 2), UNROLL, load, store, south, north)
    sweep(height, width, (0,), UNROLL, partial(load_state, middle), store_depth, south, north)


def edge_kernel(turned, got_pair, got_other, depth, top, bottom, columns, rows):
    height, width = depth.shape
    rows[...] = jnp.zeros_like(rows)
    column = lax.axis_index("gx")
    even = lax.rem(column, 2) == 0
    outside = (column == 0) | (column == lax.axis_size("gx") - 1)
    for index in range(4):
        start = index * SLOT
        own = index * SUBLANES
        rows[start : start + KEEP] = turned[own : own + KEEP]
        rows[start + SLOT - KEEP : start + SLOT] = turned[own + KEEP : own + 2 * KEEP]
        for far in range(2):
            pair = got_pair[pl.ds(4 * far + index, 1), :]
            other = jnp.where(outside, 0.0, got_other[pl.ds(4 * far + index, 1), :])
            rows[pl.ds(start + SLOT - KEEP - 1 - far, 1), :] = jnp.where(even, other, pair)
            rows[pl.ds(start + KEEP + far, 1), :] = jnp.where(even, pair, other)
    lane = lax.broadcasted_iota(jnp.int32, (SLOT, height), 1)
    state = [rows[c * SLOT : (c + 1) * SLOT] for c in range(3)]
    openness = rows[3 * SLOT : 4 * SLOT]
    wet = (openness > 0.0).astype(jnp.float32)
    damping = wet / (1.0 + time_step * openness)
    for _ in range(STEPS):
        from_east, from_west, from_south, from_north = flux_terms(*state)
        update = [
            pltpu.roll(e, SLOT - 1, 0)
            + pltpu.roll(w, 1, 0)
            + jnp.where(lane == height - 1, 0.0, pltpu.roll(s, height - 1, 1))
            + jnp.where(lane == 0, 0.0, pltpu.roll(n, 1, 1))
            for e, w, s, n in zip(from_east, from_west, from_south, from_north)
        ]
        state = [wet * update[0], damping * update[1], damping * update[2]]
    for c in range(3):
        last = (4 * c - 2) % LANES
        rows[last : last + 2] = state[c][KEEP - 2 : KEEP]
        rows[4 * c : 4 * c + 2] = state[c][SLOT - KEEP : SLOT - KEEP + 2]
    lane = lax.broadcasted_iota(jnp.int32, (LANES, LANES), 1)
    for block in range(height // LANES):
        span = slice(block * LANES, (block + 1) * LANES)
        turned_back = rows[:, span].T
        columns[span] = turned_back
        target, first = (top, 0) if block * LANES < width else (bottom, width)
        for end, chosen in ((0, lane < 2), (width - LANES, lane >= LANES - 2)):
            target[block * LANES - first : (block + 1) * LANES - first, end : end + LANES] = (
                jnp.where(chosen, turned_back, depth[span, end : end + LANES])
            )


def finish_kernel(
    top, bottom, columns, middle, damping, result, momenta, south, north, sent
):
    height, width = damping.shape
    copies = [
        pltpu.make_async_copy(top, result.at[0, 0:width], sent.at[0]),
        pltpu.make_async_copy(bottom, result.at[0, width:height], sent.at[1]),
    ]
    for copy in copies:
        copy.start()
    lane = lax.broadcasted_iota(jnp.int32, (SUBLANES, LANES), 1)
    tiles = width // LANES

    def store(group, t, update):
        span = tile_span(group, t)
        for i in range(2):
            value = damping[span] * update[i]
            if t == 0 or t == tiles - 1:
                outer = pltpu.roll(columns[rows_of(group), :], LANES - 4 * (i + 1), 1)
            if t == 0:
                value = jnp.where(lane < 2, outer, value)
            if t == tiles - 1:
                value = jnp.where(lane >= LANES - 2, outer, value)
            momenta[(i, *span)] = value

    sweep(height, width, (1, 2), FEW, partial(load_state, middle), store, south, north)
    copies.append(pltpu.make_async_copy(momenta, result.at[1:3], sent.at[2]))
    copies[-1].start()
    for copy in copies:
        copy.wait()


def place_top_kernel(tile, result, sent):
    copy = pltpu.make_async_copy(tile, result.at[0 : tile.shape[0]], sent)
    copy.start()
    copy.wait()


def place_bottom_kernel(tile, begun, result, sent):
    side = tile.shape[0]
    copy = pltpu.make_async_copy(tile, result.at[side : 2 * side], sent)
    copy.start()
    copy.wait()


def direct(top, bottom, columns, middle, damping, first, second):
    _, height, width = middle.shape
    f32 = jnp.float32

    def move(tile, distance):
        if distance == 0:
            return tile
        count = lax.axis_size("gx")
        return lax.ppermute(tile, "gx", [(i, i ^ distance) for i in range(count)])

    moved = move(top, first), move(bottom, second)
    final_fields = pl.pallas_call(
        finish_kernel,
        out_shape=pltpu.HBM(middle.shape, f32),
        in_specs=[VMEM] * 5,
        out_specs=HBM,
        scratch_shapes=[
            pltpu.VMEM((2, height, width), f32),
            pltpu.VMEM((2, width // LANES, height + SUBLANES, LANES), f32),
            pltpu.VMEM((2, width // LANES, height + SUBLANES, LANES), f32),
            pltpu.SemaphoreType.DMA((3,)),
        ],
        compiler_params=PARAMS,
        cost_estimate=pl.CostEstimate(
            flops=100 * middle.size, bytes_accessed=8 * middle.size, transcendentals=0
        ),
        name="finish",
    )(top, bottom, columns, middle, damping)
    begun = pl.pallas_call(
        place_top_kernel,
        out_shape=pltpu.HBM((height, width), f32),
        in_specs=[VMEM],
        out_specs=HBM,
        scratch_shapes=[pltpu.SemaphoreType.DMA],
        compiler_params=PARAMS,
        name="place_top",
    )(moved[0])
    owned_depth = lax.dynamic_update_slice(begun, moved[1], (width, 0))
    return final_fields, owned_depth


def other_pairs(count):
    groups = lax.axis_size("groups")
    pairs = []
    for group in range(groups):
        base = group * count
        pairs += [(base + i, base + i + 1) for i in range(1, count - 1, 2)]
        if groups % 2:
            pairs.append((base, base + count - 1))
        elif group % 2 == 0:
            pairs += [(base + end, base + count + end) for end in (0, count - 1)]
    return pairs + [(b, a) for a, b in pairs]


def in_hbm(x):
    return pltpu.with_memory_space_constraint(x, pltpu.HBM)


def body(fields, friction, wet_mask, owner_table):
    _, height, width = fields.shape
    count = lax.axis_size("gx")
    distances = 1 << LEVELS
    blocks = height // LANES
    f32 = jnp.float32
    row_payload = jax.ShapeDtypeStruct((SUBLANES, height), f32)
    fields, friction, wet_mask, turned, pay_pair, pay_other, choice = pl.pallas_call(
        pack_kernel,
        out_shape=[
            jax.ShapeDtypeStruct(fields.shape, f32),
            jax.ShapeDtypeStruct(friction.shape, f32),
            jax.ShapeDtypeStruct(wet_mask.shape, jnp.int32),
            jax.ShapeDtypeStruct((4 * SUBLANES, height), f32),
            row_payload,
            row_payload,
            pltpu.SMEM((1,), jnp.int32),
        ],
        in_specs=[HBM] * 4,
        out_specs=[VMEM] * 6 + [SMEM],
        scratch_shapes=[
            pltpu.SMEM(owner_table.shape, jnp.int32),
            pltpu.SemaphoreType.DMA((blocks, 3)),
            pltpu.SemaphoreType.DMA,
        ],
        compiler_params=PARAMS,
        name="pack",
    )(*[in_hbm(x) for x in (fields, friction, wet_mask, owner_table)])
    got_pair = lax.ppermute(pay_pair, "gx", [(i, i ^ 1) for i in range(count)])
    got_other = lax.ppermute(pay_other, ("groups", "gx"), other_pairs(count))
    stripe = jax.ShapeDtypeStruct((height, width), f32)
    depth, middle, damping = pl.pallas_call(
        main_kernel,
        out_shape=[stripe, jax.ShapeDtypeStruct(fields.shape, f32), stripe],
        in_specs=[VMEM] * 3,
        out_specs=[VMEM] * 3,
        scratch_shapes=[
            pltpu.VMEM((height, width), f32),
            pltpu.VMEM((3, width // LANES, height + SUBLANES, LANES), f32),
            pltpu.VMEM((3, width // LANES, height + SUBLANES, LANES), f32),
        ],
        compiler_params=PARAMS,
        cost_estimate=pl.CostEstimate(
            flops=200 * fields.size, bytes_accessed=16 * height * width, transcendentals=0
        ),
        name="step",
    )(fields, friction, wet_mask)
    tile = jax.ShapeDtypeStruct((width, width), f32)
    top, bottom, columns = pl.pallas_call(
        edge_kernel,
        out_shape=[tile, tile, jax.ShapeDtypeStruct((height, LANES), f32)],
        in_specs=[VMEM] * 4,
        out_specs=[VMEM] * 3,
        scratch_shapes=[pltpu.VMEM((LANES, height), f32)],
        compiler_params=PARAMS,
        name="edge_columns",
    )(turned, got_pair, got_other, depth)
    return lax.switch(
        choice[0],
        [
            partial(direct, first=first, second=second)
            for first in range(distances)
            for second in range(distances)
        ],
        top,
        bottom,
        columns,
        middle,
        damping,
    )


def solution(mesh):
    in_specs = (P(None, "groups", "gx"), P("groups", "gx"), P("groups", "gx"), P("groups", None))
    out_specs = (P(None, "groups", "gx"), P("groups", "gx"))
    return jax.shard_map(body, mesh=mesh, in_specs=in_specs, out_specs=out_specs, check_vma=False)
```

```python
from functools import partial

import jax
import jax.numpy as jnp
from jax import lax
from jax.experimental import pallas as pl
from jax.experimental.pallas import tpu as pltpu
from jax.sharding import PartitionSpec as P


STEPS = 2
LEVELS = 3
LANES = 128
SUBLANES = 8
UNROLL = 64
FEW = 2
SLOT = 16
KEEP = 4
VMEM_BYTES = 16 * 1024 * 1024

depth_floor = 0.25
flux_factor = 0.1
time_step = 0.25

VMEM = pl.BlockSpec(memory_space=pltpu.VMEM)
HBM = pl.BlockSpec(memory_space=pltpu.HBM)
SMEM = pl.BlockSpec(memory_space=pltpu.SMEM)
PARAMS = pltpu.CompilerParams(vmem_limit_bytes=VMEM_BYTES)


def flux_terms(depth, east, south):
    inverse = flux_factor / jnp.maximum(depth, depth_floor)
    speed_east = inverse * east
    speed_south = inverse * south
    pressure = (0.5 * flux_factor) * depth * depth
    cross = south * speed_east
    flux_east = (flux_factor * east, east * speed_east + pressure, cross)
    flux_south = (flux_factor * south, cross, south * speed_south + pressure)
    quarter = (0.25 * depth, 0.25 * east, 0.25 * south)
    from_east = [a - f for a, f in zip(quarter, flux_east)]
    from_west = [a + f for a, f in zip(quarter, flux_east)]
    from_south = [a - g for a, g in zip(quarter, flux_south)]
    from_north = [a + g for a, g in zip(quarter, flux_south)]
    return from_east, from_west, from_south, from_north


def pack_kernel(
    fields_in, friction_in, mask_in, table_in,
    fields, friction, wet_mask, turned, pay_pair, pay_other, choice,
    table, arrived, told,
):
    height, width = fields.shape[1], fields.shape[2]
    count = height // LANES
    read_table = pltpu.make_async_copy(table_in, table, told)
    read_table.start()
    copies = []
    for block in range(count):
        span = pl.ds(block * LANES, LANES)
        copies.append(
            [
                pltpu.make_async_copy(fields_in.at[:, span], fields.at[:, span], arrived.at[block, 0]),
                pltpu.make_async_copy(friction_in.at[span], friction.at[span], arrived.at[block, 1]),
                pltpu.make_async_copy(mask_in.at[span], wet_mask.at[span], arrived.at[block, 2]),
            ]
        )
        for copy in copies[-1]:
            copy.start()
    read_table.wait()
    column = lax.axis_index("gx")
    key = 0
    for tile_row in range(table.shape[0]):
        key = (key << LEVELS) + (table[tile_row, column] ^ column)
    choice[0] = key
    lane = lax.broadcasted_iota(jnp.int32, (LANES, LANES), 1)
    ends = (slice(0, LANES), slice(width - LANES, width))

    def outer(left, right):
        return jnp.where(lane < KEEP, left, right)

    for block in range(count):
        for copy in copies[block]:
            copy.wait()
        span = slice(block * LANES, (block + 1) * LANES)
        openness = outer(
            *[wet_mask[span, end].astype(jnp.float32) * friction[span, end] for end in ends]
        )
        wet = (openness > 0.0).astype(jnp.float32)
        packed = openness
        for c in range(3):
            value = outer(*[fields[c, span, end] for end in ends]) * wet
            value = pltpu.roll(value, (c - 3) * SUBLANES % LANES, 1)
            start = (c - 3) * SUBLANES - KEEP + LANES
            packed = jnp.where((lane >= start) & (lane < start + SUBLANES), value, packed)
        packed = pltpu.roll(packed, 3 * SUBLANES + KEEP, 1)
        turned[:, span] = packed.T[0 : 4 * SUBLANES]
    even = lax.rem(lax.axis_index("gx"), 2) == 0
    for index in range(4):
        for far in range(2):
            right = turned[pl.ds(index * SUBLANES + KEEP - 1 - far, 1), :]
            left = turned[pl.ds(index * SUBLANES + KEEP + far, 1), :]
            pay_pair[pl.ds(4 * far + index, 1), :] = jnp.where(even, right, left)
            pay_other[pl.ds(4 * far + index, 1), :] = jnp.where(even, left, right)


def rows_of(group, offset=0):
    start = group * SUBLANES
    if not isinstance(start, int):
        start = pl.multiple_of(start, SUBLANES)
    return pl.ds(start + offset, SUBLANES)


def sweep(height, width, parts, unroll, load, store, south, north):
    groups = height // SUBLANES
    tiles = width // LANES
    lane = lax.broadcasted_iota(jnp.int32, (SUBLANES, LANES), 1)
    first_lane, last_lane = lane == 0, lane == LANES - 1
    zero = jnp.zeros((SUBLANES, LANES), jnp.float32)
    for i in range(len(parts)):
        for t in range(tiles):
            north[i, t, 0:SUBLANES] = zero
            south[i, t, height : height + SUBLANES] = zero

    def across(from_east, from_west):
        east = [pltpu.roll(x, LANES - 1, 1) for x in from_east]
        west = [pltpu.roll(x, 1, 1) for x in from_west]
        return [
            jnp.where(last_lane, east[(t + 1) % tiles], east[t])
            + jnp.where(first_lane, west[t - 1], west[t])
            for t in range(tiles)
        ]

    def finish(group, held):
        for t in range(tiles):
            below = [south[i, t, rows_of(group, 1)] for i in range(len(parts))]
            store(group, t, [held[i][t] + below[i] for i in range(len(parts))])

    def one(group, held):
        per_tile = [flux_terms(*state) for state in load(group)]
        for t in range(tiles):
            for i, part in enumerate(parts):
                south[i, t, rows_of(group)] = per_tile[t][2][part]
                north[i, t, rows_of(group + 1)] = per_tile[t][3][part]
        finish(jnp.maximum(group - 1, 0), held)
        held = []
        for i, part in enumerate(parts):
            side = across([x[0][part] for x in per_tile], [x[1][part] for x in per_tile])
            held.append([side[t] + north[i, t, rows_of(group, SUBLANES - 1)] for t in range(tiles)])
        return held

    def trip(k, held):
        for j in range(unroll):
            held = one(k * unroll + j, held)
        return held

    held = lax.fori_loop(0, groups // unroll, trip, [[zero] * tiles] * len(parts))
    finish(groups - 1, held)


def tile_span(group, t):
    return (rows_of(group), slice(t * LANES, (t + 1) * LANES))


def load_state(middle, group):
    tiles = middle.shape[2] // LANES
    return [[middle[(c, *tile_span(group, t))] for c in range(3)] for t in range(tiles)]


def main_kernel(fields, friction, wet_mask, depth, middle, damping, wet_cells, south, north):
    height, width = depth.shape
    tiles = width // LANES

    def load(group):
        states = []
        for t in range(tiles):
            span = tile_span(group, t)
            openness = wet_mask[span].astype(jnp.float32) * friction[span]
            wet = (openness > 0.0).astype(jnp.float32)
            wet_cells[span] = wet
            damping[span] = wet / (1.0 + time_step * openness)
            states.append([fields[(c, *span)] * wet for c in range(3)])
        return states

    def store(group, t, update):
        span = tile_span(group, t)
        damp = damping[span]
        middle[(0, *span)] = wet_cells[span] * update[0]
        middle[(1, *span)] = damp * update[1]
        middle[(2, *span)] = damp * update[2]

    def store_depth(group, t, update):
        span = tile_span(group, t)
        depth[span] = wet_cells[span] * update[0]

    sweep(height, width, (0, 1, 2), UNROLL, load, store, south, north)
    sweep(height, width, (0,), UNROLL, partial(load_state, middle), store_depth, south, north)


def edge_kernel(turned, got_pair, got_other, depth, top, bottom, columns, rows):
    height, width = depth.shape
    rows[...] = jnp.zeros_like(rows)
    column = lax.axis_index("gx")
    even = lax.rem(column, 2) == 0
    outside = (column == 0) | (column == lax.axis_size("gx") - 1)
    for index in range(4):
        start = index * SLOT
        own = index * SUBLANES
        rows[start : start + KEEP] = turned[own : own + KEEP]
        rows[start + SLOT - KEEP : start + SLOT] = turned[own + KEEP : own + 2 * KEEP]
        for far in range(2):
            pair = got_pair[pl.ds(4 * far + index, 1), :]
            other = jnp.where(outside, 0.0, got_other[pl.ds(4 * far + index, 1), :])
            rows[pl.ds(start + SLOT - KEEP - 1 - far, 1), :] = jnp.where(even, other, pair)
            rows[pl.ds(start + KEEP + far, 1), :] = jnp.where(even, pair, other)
    lane = lax.broadcasted_iota(jnp.int32, (SLOT, height), 1)
    state = [rows[c * SLOT : (c + 1) * SLOT] for c in range(3)]
    openness = rows[3 * SLOT : 4 * SLOT]
    wet = (openness > 0.0).astype(jnp.float32)
    damping = wet / (1.0 + time_step * openness)
    for _ in range(STEPS):
        from_east, from_west, from_south, from_north = flux_terms(*state)
        update = [
            pltpu.roll(e, SLOT - 1, 0)
            + pltpu.roll(w, 1, 0)
            + jnp.where(lane == height - 1, 0.0, pltpu.roll(s, height - 1, 1))
            + jnp.where(lane == 0, 0.0, pltpu.roll(n, 1, 1))
            for e, w, s, n in zip(from_east, from_west, from_south, from_north)
        ]
        state = [wet * update[0], damping * update[1], damping * update[2]]
    for c in range(3):
        last = (4 * c - 2) % LANES
        rows[last : last + 2] = state[c][KEEP - 2 : KEEP]
        rows[4 * c : 4 * c + 2] = state[c][SLOT - KEEP : SLOT - KEEP + 2]
    lane = lax.broadcasted_iota(jnp.int32, (LANES, LANES), 1)
    for block in range(height // LANES):
        span = slice(block * LANES, (block + 1) * LANES)
        turned_back = rows[:, span].T
        columns[span] = turned_back
        target, first = (top, 0) if block * LANES < width else (bottom, width)
        for end, chosen in ((0, lane < 2), (width - LANES, lane >= LANES - 2)):
            target[block * LANES - first : (block + 1) * LANES - first, end : end + LANES] = (
                jnp.where(chosen, turned_back, depth[span, end : end + LANES])
            )


def finish_kernel(
    top, bottom, columns, middle, damping, result, momenta, south, north, sent
):
    height, width = damping.shape
    copies = [
        pltpu.make_async_copy(top, result.at[0, 0:width], sent.at[0]),
        pltpu.make_async_copy(bottom, result.at[0, width:height], sent.at[1]),
    ]
    for copy in copies:
        copy.start()
    lane = lax.broadcasted_iota(jnp.int32, (SUBLANES, LANES), 1)
    tiles = width // LANES

    def store(group, t, update):
        span = tile_span(group, t)
        for i in range(2):
            value = damping[span] * update[i]
            if t == 0 or t == tiles - 1:
                outer = pltpu.roll(columns[rows_of(group), :], LANES - 4 * (i + 1), 1)
            if t == 0:
                value = jnp.where(lane < 2, outer, value)
            if t == tiles - 1:
                value = jnp.where(lane >= LANES - 2, outer, value)
            momenta[(i, *span)] = value

    sweep(height, width, (1, 2), FEW, partial(load_state, middle), store, south, north)
    copies.append(pltpu.make_async_copy(momenta, result.at[1:3], sent.at[2]))
    copies[-1].start()
    for copy in copies:
        copy.wait()


def place_top_kernel(tile, result, sent):
    copy = pltpu.make_async_copy(tile, result.at[0 : tile.shape[0]], sent)
    copy.start()
    copy.wait()


def direct(top, bottom, columns, middle, damping, first, second):
    _, height, width = middle.shape
    f32 = jnp.float32

    def move(tile, distance):
        if distance == 0:
            return tile
        count = lax.axis_size("gx")
        return lax.ppermute(tile, "gx", [(i, i ^ distance) for i in range(count)])

    moved = move(top, first), move(bottom, second)
    final_fields = pl.pallas_call(
        finish_kernel,
        out_shape=pltpu.HBM(middle.shape, f32),
        in_specs=[VMEM] * 5,
        out_specs=HBM,
        scratch_shapes=[
            pltpu.VMEM((2, height, width), f32),
            pltpu.VMEM((2, width // LANES, height + SUBLANES, LANES), f32),
            pltpu.VMEM((2, width // LANES, height + SUBLANES, LANES), f32),
            pltpu.SemaphoreType.DMA((3,)),
        ],
        compiler_params=PARAMS,
        cost_estimate=pl.CostEstimate(
            flops=100 * middle.size, bytes_accessed=8 * middle.size, transcendentals=0
        ),
        name="finish",
    )(top, bottom, columns, middle, damping)
    begun = pl.pallas_call(
        place_top_kernel,
        out_shape=pltpu.HBM((height, width), f32),
        in_specs=[VMEM],
        out_specs=HBM,
        scratch_shapes=[pltpu.SemaphoreType.DMA],
        compiler_params=PARAMS,
        name="place_top",
    )(moved[0])
    owned_depth = lax.dynamic_update_slice(begun, moved[1], (width, 0))
    return final_fields, owned_depth


def other_pairs(count):
    groups = lax.axis_size("groups")
    pairs = []
    for group in range(groups):
        base = group * count
        pairs += [(base + i, base + i + 1) for i in range(1, count - 1, 2)]
        if groups % 2:
            pairs.append((base, base + count - 1))
        elif group % 2 == 0:
            pairs += [(base + end, base + count + end) for end in (0, count - 1)]
    return pairs + [(b, a) for a, b in pairs]


def in_hbm(x):
    return pltpu.with_memory_space_constraint(x, pltpu.HBM)


def body(fields, friction, wet_mask, owner_table):
    _, height, width = fields.shape
    count = lax.axis_size("gx")
    distances = 1 << LEVELS
    blocks = height // LANES
    f32 = jnp.float32
    row_payload = jax.ShapeDtypeStruct((SUBLANES, height), f32)
    fields, friction, wet_mask, turned, pay_pair, pay_other, choice = pl.pallas_call(
        pack_kernel,
        out_shape=[
            jax.ShapeDtypeStruct(fields.shape, f32),
            jax.ShapeDtypeStruct(friction.shape, f32),
            jax.ShapeDtypeStruct(wet_mask.shape, jnp.int32),
            jax.ShapeDtypeStruct((4 * SUBLANES, height), f32),
            row_payload,
            row_payload,
            pltpu.SMEM((1,), jnp.int32),
        ],
        in_specs=[HBM] * 4,
        out_specs=[VMEM] * 6 + [SMEM],
        scratch_shapes=[
            pltpu.SMEM(owner_table.shape, jnp.int32),
            pltpu.SemaphoreType.DMA((blocks, 3)),
            pltpu.SemaphoreType.DMA,
        ],
        compiler_params=PARAMS,
        name="pack",
    )(*[in_hbm(x) for x in (fields, friction, wet_mask, owner_table)])
    got_other = lax.ppermute(pay_other, ("groups", "gx"), other_pairs(count))
    got_pair = lax.ppermute(pay_pair, "gx", [(i, i ^ 1) for i in range(count)])
    stripe = jax.ShapeDtypeStruct((height, width), f32)
    depth, middle, damping = pl.pallas_call(
        main_kernel,
        out_shape=[stripe, jax.ShapeDtypeStruct(fields.shape, f32), stripe],
        in_specs=[VMEM] * 3,
        out_specs=[VMEM] * 3,
        scratch_shapes=[
            pltpu.VMEM((height, width), f32),
            pltpu.VMEM((3, width // LANES, height + SUBLANES, LANES), f32),
            pltpu.VMEM((3, width // LANES, height + SUBLANES, LANES), f32),
        ],
        compiler_params=PARAMS,
        cost_estimate=pl.CostEstimate(
            flops=200 * fields.size, bytes_accessed=16 * height * width, transcendentals=0
        ),
        name="step",
    )(fields, friction, wet_mask)
    tile = jax.ShapeDtypeStruct((width, width), f32)
    top, bottom, columns = pl.pallas_call(
        edge_kernel,
        out_shape=[tile, tile, jax.ShapeDtypeStruct((height, LANES), f32)],
        in_specs=[VMEM] * 4,
        out_specs=[VMEM] * 3,
        scratch_shapes=[pltpu.VMEM((LANES, height), f32)],
        compiler_params=PARAMS,
        name="edge_columns",
    )(turned, got_pair, got_other, depth)
    return lax.switch(
        choice[0],
        [
            partial(direct, first=first, second=second)
            for first in range(distances)
            for second in range(distances)
        ],
        top,
        bottom,
        columns,
        middle,
        damping,
    )


def solution(mesh):
    in_specs = (P(None, "groups", "gx"), P("groups", "gx"), P("groups", "gx"), P("groups", None))
    out_specs = (P(None, "groups", "gx"), P("groups", "gx"))
    return jax.shard_map(body, mesh=mesh, in_specs=in_specs, out_specs=out_specs, check_vma=False)
```
